32 devices in a mesh: section: 16 (over z, x, core), dp: 2 (over y).
Axes of the slice: x: 2, y: 2, z: 4, core: 2. Of those that a mesh axis runs over, the one named last changes fastest.
Arguments:
- w_value: bfloat16 [16, 2, 4608, 1024], P('section', None, None, 'dp'), may hold values from -0.09375 to 0.09375
- w_out: bfloat16 [16, 2, 1024, 4608], P('section', None, 'dp'), may hold values from -0.1875 to 0.1875
- norm_gain: float32 [16, 2, 4608], P('section'), may hold values from 0.5 to 1.5
- saved_inputs: bfloat16 [16, 3, 2, 16, 4608], P('section', None, None, 'dp'), may hold values from -6 to 6
- arriving: bfloat16 [16, 2, 16, 4608], P('section', None, 'dp'), may hold values from -6 to 6
- returning: bfloat16 [16, 2, 16, 4608], P('section', None, 'dp'), may hold values from -6 to 6
- fresh_rows: bfloat16 [4, 16, 4608], P(None, 'dp'), may hold values from -6 to 6
- targets: bfloat16 [4, 16, 4608], P(None, 'dp'), may hold values from -6 to 6
- fill_slots: int32 [16, 4, 2], P('section'), may hold values from 0 to 2
- read_slots: int32 [16, 4, 2], P('section'), may hold values from 0 to 2
Outputs:
- activ_out: bfloat16 [16, 2, 16, 4608], P('section', None, 'dp')
- cotan_out: bfloat16 [16, 2, 16, 4608], P('section', None, 'dp')
- stash_out: bfloat16 [16, 3, 2, 16, 4608], P('section', None, None, 'dp')
- grad_value: bfloat16 [16, 2, 4608, 1024], P('section', None, None, 'dp')
- grad_out: bfloat16 [16, 2, 1024, 4608], P('section', None, 'dp')
- grad_gain: float32 [16, 2, 4608], P('section')
The draws below stay inside these ranges and needn't reach their ends.
All inputs are finite; a program needn't handle non-finite values.
Results may differ from the reference program's by a relative error of at most 0.029.
Values may be sent and summed in bfloat16 or wider, within the bound.
A program may use at most 192 MiB of HBM per device.

```python
import jax
import jax.numpy as jnp
from jax import lax

D = 4608
K = 1024
TICKS = 4
SLOTS = 3
ROWS = 16
N_SECTION = 16
N_DP = 2


def set_ends(drawn, stream_key, smallest, top_value):
    extent = drawn.shape
    place = [jax.random.randint(jax.random.fold_in(stream_key, axis), (), 0, extent[axis]) for axis in range(len(extent))]
    drawn = drawn.at[tuple(place)].set(smallest)
    longest = extent.index(max(extent))
    place[longest] = (place[longest] + 1) % extent[longest]
    return drawn.at[tuple(place)].set(top_value)


def block_scale(rng, dims, cuts, low, high):
    gain, own = 1.0, jax.random.fold_in(rng, 6)
    for position, shards_of in cuts:
        steps = jnp.exp(jax.random.uniform(jax.random.fold_in(own, position), (shards_of,), jnp.float32, low / len(cuts), high / len(cuts)))
        gain = gain * jnp.repeat(steps, dims[position] // shards_of).reshape([-1 if axis == position else 1 for axis in range(len(dims))])
    return gain


def scatter_about(key, shape, deviation, reach, cuts=(), held_as=jnp.bfloat16):
    values = jax.random.normal(key, shape, jnp.float32) * deviation
    if len(cuts) > 0:
        values = block_scale(key, shape, cuts, -0.22, 0.18) * values
    return jnp.clip(values, min=-reach, max=reach).astype(held_as)


def setup_inputs(seed: int = 0) -> dict:
    key_of = jax.random.split(jax.random.key(seed), 11)
    w_value = scatter_about(key_of[0], (N_SECTION, 2, D, K), D ** -0.5, 0.09375, ((0, 16), (3, 2)))
    w_out = scatter_about(key_of[1], (N_SECTION, 2, K, D), K ** -0.5, 0.1875, ((0, 16), (2, 2)))
    norm_gain = jnp.clip(1.0 + 0.1 * jax.random.normal(key_of[2], (N_SECTION, 2, D), jnp.float32), 0.5, 1.5)
    saved_inputs = scatter_about(key_of[3], (N_SECTION, SLOTS, 2, ROWS, D), 1.0, 6.0, ((0, 16), (3, 2)))
    arriving = scatter_about(key_of[4], (N_SECTION, 2, ROWS, D), 1.0, 6.0, ((0, 16), (2, 2)))
    returning = scatter_about(key_of[5], (N_SECTION, 2, ROWS, D), 1.0, 6.0, ((0, 16), (2, 2)))
    fresh_rows = scatter_about(key_of[6], (TICKS, ROWS, D), 1.0, 6.0, ((1, 2),))
    targets = scatter_about(key_of[7], (TICKS, ROWS, D), 1.0, 6.0, ((1, 2),))
    fill_slots = set_ends(jax.random.randint(key_of[8], (N_SECTION, TICKS, 2), 0, SLOTS), jax.random.fold_in(key_of[8], 1), 0, SLOTS - 1).astype(jnp.int32)
    read_slots = set_ends(jax.random.randint(key_of[9], (N_SECTION, TICKS, 2), 0, SLOTS), jax.random.fold_in(key_of[9], 1), 0, SLOTS - 1).astype(jnp.int32)
    return dict(w_value=w_value, w_out=w_out, norm_gain=norm_gain, saved_inputs=saved_inputs, arriving=arriving, returning=returning, fresh_rows=fresh_rows, targets=targets, fill_slots=fill_slots, read_slots=read_slots)


epsilon = 1e-06

def exact_dot(left, right):
    return jnp.dot(left.astype(jnp.float32), right.astype(jnp.float32), precision=lax.Precision.HIGHEST)

def normalize(block_rows, gain_row):
    values = block_rows.astype(jnp.float32)
    inv_root = lax.rsqrt(lax.optimization_barrier(jnp.mean(values * values, axis=-1, keepdims=True)) + epsilon)
    scaled = values * inv_root
    return (scaled, inv_root, (scaled * gain_row).astype(jnp.bfloat16))

def shard_sums(left, right):
    pieces = right.shape[0] // N_DP
    split_left = left.astype(jnp.float32).reshape(left.shape[0], N_DP, pieces)
    split_right = right.astype(jnp.float32).reshape(N_DP, pieces, right.shape[1])
    terms = jnp.einsum('rjk,jkd->jrd', split_left, split_right, precision=lax.Precision.HIGHEST)
    rounded = lax.optimization_barrier(terms.astype(jnp.bfloat16))
    return lax.optimization_barrier(jnp.sum(rounded.astype(jnp.float32), axis=0))

def forward_layer(block_rows, gain_row, value_mat, out_mat):
    scaled, inv_root, normed = normalize(block_rows, gain_row)
    values = exact_dot(normed, value_mat).astype(jnp.bfloat16)
    return (block_rows.astype(jnp.float32) + shard_sums(values, out_mat)).astype(jnp.bfloat16)

def backward_layer(source, upstream, gain_row, value_mat, out_mat):
    scaled, inv_root, normed = normalize(source, gain_row)
    down_grad = exact_dot(upstream, out_mat.T).astype(jnp.bfloat16)
    pulled = shard_sums(down_grad, value_mat.T)
    weighted = pulled * gain_row
    inner_mean = lax.optimization_barrier(jnp.mean(weighted * scaled, axis=-1, keepdims=True))
    grad_in = (upstream.astype(jnp.float32) + inv_root * (weighted - scaled * inner_mean)).astype(jnp.bfloat16)
    values = exact_dot(normed, value_mat).astype(jnp.bfloat16)
    return (grad_in, exact_dot(normed.T, down_grad), exact_dot(values.T, upstream), lax.optimization_barrier(jnp.sum(pulled * scaled, axis=0)))

def section_work(entries):
    inputs_now, upstream_now, sources, gains, value_mats, out_mats = entries
    layer_outs, grad_ins, value_terms, out_terms, gain_terms = ([], [], [], [], [])
    for group in range(2):
        layer_outs.append(forward_layer(inputs_now[group], gains[group], value_mats[group], out_mats[group]))
        grad_in, value_term, out_term, gain_term = backward_layer(sources[group], upstream_now[group], gains[group], value_mats[group], out_mats[group])
        grad_ins.append(grad_in)
        value_terms.append(value_term)
        out_terms.append(out_term)
        gain_terms.append(gain_term)
    return (jnp.stack(layer_outs), jnp.stack(grad_ins), jnp.stack(value_terms), jnp.stack(out_terms), jnp.stack(gain_terms))

def reference(w_value, w_out, norm_gain, saved_inputs, arriving, returning, fresh_rows, targets, fill_slots, read_slots):
    activations = arriving
    cotangents = returning
    saved = saved_inputs
    value_sums = jnp.zeros(w_value.shape, jnp.float32)
    out_sums = jnp.zeros(w_out.shape, jnp.float32)
    gain_sums = jnp.zeros(norm_gain.shape, jnp.float32)
    slot_ids = jnp.arange(SLOTS, dtype=jnp.int32)
    outputs = activations
    gradients = cotangents
    for tick_index in range(TICKS):
        if tick_index > 0:
            lower_group = jnp.concatenate([fresh_rows[tick_index][None], outputs[:-1, 0]], axis=0)
            upper_group = jnp.concatenate([outputs[-1:, 0], outputs[:-1, 1]], axis=0)
            activations = jnp.stack([lower_group, upper_group], axis=1)
            finish = (outputs[-1, 1].astype(jnp.float32) - targets[tick_index - 1].astype(jnp.float32)).astype(jnp.bfloat16)
            lower_grad = jnp.concatenate([gradients[1:, 0], gradients[:1, 1]], axis=0)
            upper_grad = jnp.concatenate([gradients[1:, 1], finish[None]], axis=0)
            cotangents = jnp.stack([lower_grad, upper_grad], axis=1)
        written = slot_ids[None, :, None] == fill_slots[:, tick_index, :][:, None, :]
        saved = jnp.where(written[:, :, :, None, None], activations[:, None], saved)
        chosen = slot_ids[None, :, None] == read_slots[:, tick_index, :][:, None, :]
        sources = lax.optimization_barrier(jnp.sum(jnp.where(chosen[:, :, :, None, None], saved.astype(jnp.float32), jnp.zeros((), jnp.float32)), axis=1)).astype(jnp.bfloat16)
        outputs, gradients, value_terms, out_terms, gain_terms = lax.map(section_work, (activations, cotangents, sources, norm_gain, w_value, w_out))
        value_sums = value_sums + value_terms
        out_sums = out_sums + out_terms
        gain_sums = gain_sums + gain_terms
    grad_scale = (TICKS * ROWS) ** (-0.5)
    return (outputs, gradients, saved, (value_sums * grad_scale).astype(jnp.bfloat16), (out_sums * grad_scale).astype(jnp.bfloat16), gain_sums * grad_scale)
```

```python
import functools

import jax
import jax.numpy as jnp
from jax import lax
from jax.experimental import pallas as pl
from jax.experimental.pallas import tpu as pltpu
from jax.sharding import PartitionSpec as P

epsilon = 1e-06


def shifted(shard, axis, by):
    devices = lax.axis_size(axis)
    return lax.ppermute(shard, axis, [(i, (i + by) % devices) for i in range(devices)])


def normalize(block_rows, gain_row):
    values = block_rows.astype(jnp.float32)
    inv_root = lax.rsqrt(jnp.mean(values * values, axis=-1, keepdims=True) + epsilon)
    scaled = values * inv_root
    return (scaled, inv_root, (scaled * gain_row).astype(jnp.bfloat16))


def times_transposed(left, right):
    return lax.dot_general(
        left, right, (((1,), (1,)), ((), ())), preferred_element_type=jnp.float32
    )


def transposed_times(left, right):
    return lax.dot_general(
        left, right, (((0,), (0,)), ((), ())), preferred_element_type=jnp.float32
    )


def weight_terms(value_group, normed_all, down_grad, upstream_all):
    values = jnp.dot(normed_all, value_group, preferred_element_type=jnp.float32).astype(
        jnp.bfloat16
    )
    return (transposed_times(normed_all, down_grad), transposed_times(values, upstream_all))


def body(
    w_value,
    w_out,
    norm_gain,
    saved_inputs,
    arriving,
    returning,
    fresh_rows,
    targets,
    fill_slots,
    read_slots,
):
    value_mats = w_value[0]
    out_mats = w_out[0]
    gains = norm_gain[0]
    saved = saved_inputs[0]
    activations = arriving[0]
    cotangents = returning[0]
    tick_count = fresh_rows.shape[0]
    tok_rows = activations.shape[1]
    all_rows = tok_rows * lax.axis_size("dp")
    section_index = lax.axis_index("section")
    last_section = lax.axis_size("section") - 1
    row_offset = lax.axis_index("dp") * tok_rows
    activations, new_rows = (
        lax.all_gather(activations, "dp", axis=1, tiled=True),
        lax.all_gather(fresh_rows, "dp", axis=1, tiled=True),
    )

    def own_rows(block):
        return lax.dynamic_slice_in_dim(block, row_offset, tok_rows, 0)

    def forward(block, group):
        scaled, inv_root, normed = normalize(block, gains[group])
        values = jnp.dot(normed, value_mats[group], preferred_element_type=jnp.float32).astype(
            jnp.bfloat16
        )
        summed = lax.psum(
            jnp.dot(values, out_mats[group], preferred_element_type=jnp.float32).astype(
                jnp.bfloat16
            ),
            "dp",
        ).astype(jnp.float32)
        return (block.astype(jnp.float32) + summed).astype(jnp.bfloat16)

    value_sums = [jnp.zeros(value_mats.shape[1:], jnp.float32) for group in range(2)]
    out_sums = [jnp.zeros(out_mats.shape[1:], jnp.float32) for group in range(2)]
    gain_sums = [jnp.zeros(gains.shape[1:], jnp.float32) for group in range(2)]
    outputs = activations
    gradients = cotangents
    for tick_index in range(tick_count):
        if tick_index > 0:
            received = shifted(outputs, "section", 1)
            lower_group = jnp.where(section_index == 0, new_rows[tick_index], received[0])
            upper_group = jnp.where(section_index == 0, received[0], received[1])
            activations = jnp.stack([lower_group, upper_group])
            returned = shifted(gradients, "section", -1)
            finish = (
                own_rows(outputs[1]).astype(jnp.float32)
                - targets[tick_index - 1].astype(jnp.float32)
            ).astype(jnp.bfloat16)
            cotangents = jnp.stack(
                [
                    jnp.where(section_index == last_section, returned[1], returned[0]),
                    jnp.where(section_index == last_section, finish, returned[1]),
                ]
            )
        for group in range(2):
            saved = saved.at[fill_slots[0, tick_index, group], group].set(
                own_rows(activations[group])
            )
        outputs = jnp.stack([forward(activations[0], 0), forward(activations[1], 1)])
        fresh_grads = []
        for group in range(2):
            source = saved[read_slots[0, tick_index, group], group]
            scaled, inv_root, normed = normalize(source, gains[group])
            normed_all, upstream_all = (
                lax.all_gather(normed, "dp", axis=0, tiled=True),
                lax.all_gather(cotangents[group], "dp", axis=0, tiled=True),
            )
            down_grad = times_transposed(upstream_all, out_mats[group]).astype(jnp.bfloat16)
            pulled = lax.psum_scatter(
                times_transposed(down_grad, value_mats[group]).astype(jnp.bfloat16),
                "dp",
                scatter_dimension=0,
                tiled=True,
            ).astype(jnp.float32)
            weighted = pulled * gains[group]
            inner_mean = jnp.mean(weighted * scaled, axis=-1, keepdims=True)
            fresh_grads.append(
                (
                    cotangents[group].astype(jnp.float32)
                    + inv_root * (weighted - scaled * inner_mean)
                ).astype(jnp.bfloat16)
            )
            gain_sums[group] = gain_sums[group] + jnp.sum(pulled * scaled, axis=0)
            value_term, out_term = weight_terms(
                value_mats[group], normed_all, down_grad, upstream_all
            )
            value_sums[group] = value_sums[group] + value_term
            out_sums[group] = out_sums[group] + out_term
        gradients = jnp.stack(fresh_grads)
    grad_scale = (tick_count * all_rows) ** (-0.5)
    gain_total = lax.psum(jnp.stack(gain_sums).astype(jnp.bfloat16), "dp").astype(jnp.float32)
    final_rows = jnp.stack([own_rows(outputs[0]), own_rows(outputs[1])])
    return (
        final_rows[None],
        gradients[None],
        saved[None],
        (jnp.stack(value_sums) * grad_scale).astype(jnp.bfloat16)[None],
        (jnp.stack(out_sums) * grad_scale).astype(jnp.bfloat16)[None],
        (gain_total * grad_scale)[None],
    )


CHUNK = 512
VMEM_GRANT = 60 * 1024 * 1024
MESH = pl.DeviceIdType.MESH


def chunk_loop(width, step):
    size = CHUNK if width % CHUNK == 0 else width
    lax.fori_loop(0, width // size, lambda i, _: step(pl.ds(pl.multiple_of(i * size, size), size)), None, unroll=UNROLL)


UNROLL = 9


def contract_sum(width, term, shape):
    size = CHUNK if width % CHUNK == 0 else width

    def step(i, total):
        return total + term(pl.ds(pl.multiple_of(i * size, size), size))

    return lax.fori_loop(0, width // size, step, jnp.zeros(shape, jnp.float32), unroll=UNROLL)


def relay_kernel(
    sections,
    wv_hbm,
    wo_hbm,
    gain_ref,
    saved_ref,
    arriving_ref,
    returning_ref,
    fresh_ref,
    targets_ref,
    fill_ref,
    read_ref,
    activ_ref,
    cotan_ref,
    stash_out_ref,
    normed_ref,
    down_ref,
    vals_ref,
    up_ref,
    gain_out_ref,
    wv,
    wo,
    xin,
    cot,
    stash,
    tgt,
    psend,
    precv,
    moved,
    lhs,
    w_sem,
    init_send,
    init_recv,
    ex_send,
    ex_recv,
    sh_send,
    sh_recv,
):
    s = lax.axis_index("section")
    d = lax.axis_index("dp")
    peer = 1 - d
    after = lax.rem(s + 1, sections)
    before = lax.rem(s + sections - 1, sections)
    is_last = s // (sections - 1)
    is_first = before // (sections - 1)
    ticks = fresh_ref.shape[0]
    half, width = arriving_ref.shape[1:]
    rows = 2 * half
    features = wv.shape[2]
    slots = saved_ref.shape[0]

    weight_copies = []
    for group in range(2):
        weight_copies.append(pltpu.make_async_copy(wv_hbm.at[group], wv.at[group], w_sem.at[group, 0]))
        weight_copies.append(pltpu.make_async_copy(wo_hbm.at[group], wo.at[group], w_sem.at[group, 1]))
    for copy in weight_copies:
        copy.start()

    barrier = pltpu.get_barrier_semaphore()
    for target in ((s, peer), (after, d), (before, d)):
        pl.semaphore_signal(barrier, inc=1, device_id=target, device_id_type=MESH)
    pl.semaphore_wait(barrier, 3)

    def to_peer(src, dst, send, recv):
        return pltpu.make_async_remote_copy(
            src_ref=src, dst_ref=dst, send_sem=send, recv_sem=recv,
            device_id=(s, peer), device_id_type=MESH,
        )

    def initial(index, src, dst):
        return to_peer(src, dst, init_send.at[index], init_recv.at[index])

    first_in = initial(0, arriving_ref, xin.at[0, pl.ds(0, 2), d])
    first_cot = initial(1, returning_ref, cot.at[0, pl.ds(0, 2), d])
    first_stash = initial(2, saved_ref, stash.at[:, :, d])
    fresh_copy = initial(3, fresh_ref.at[pl.ds(1, ticks - 1)], xin.at[pl.ds(1, ticks - 1), 2, d])
    target_copy = initial(4, targets_ref, tgt.at[:, d])
    first_in.start()
    first_cot.start()

    @pl.when(s == 0)
    def _():
        fresh_copy.start()

    @pl.when(s == sections - 1)
    def _():
        target_copy.start()

    first_stash.start()
    for group in range(2):
        xin[0, group, d] = arriving_ref[group]
        cot[0, group, d] = returning_ref[group]
        for slot in range(slots):
            stash[slot, group, d] = saved_ref[slot, group]
    for tick in range(1, ticks):
        xin[tick, 2, d] = fresh_ref[tick]
    for tick in range(ticks):
        tgt[tick, d] = targets_ref[tick]
    gain_out_ref[...] = jnp.zeros_like(gain_out_ref)

    def whole(block):
        return block.astype(jnp.float32).reshape(rows, width)

    def parted(block):
        return block.reshape(2, half, width).astype(jnp.bfloat16)

    def exchange(tick, stream):
        return to_peer(
            psend.at[tick, stream], precv.at[tick, stream],
            ex_send.at[tick, stream], ex_recv.at[tick, stream],
        )

    def shift(tick, stream):
        group = stream % 2
        if stream < 2:
            place, target, buffer = (group + is_last) % 2, after, xin
        else:
            place, target, buffer = (group + is_first) % 2, before, cot
        return pltpu.make_async_remote_copy(
            src_ref=moved.at[tick, stream], dst_ref=buffer.at[tick + 1, place],
            send_sem=sh_send.at[tick, stream], recv_sem=sh_recv.at[tick + 1, stream - group + place],
            device_id=(target, d), device_id_type=MESH,
        )

    def shift_arrival(tick, stream):
        buffer = xin if stream < 2 else cot
        return pltpu.make_async_remote_copy(
            src_ref=moved.at[0, stream], dst_ref=buffer.at[tick, stream % 2],
            send_sem=sh_send.at[0, stream], recv_sem=sh_recv.at[tick, stream],
            device_id=(after, d), device_id_type=MESH,
        )

    def input_block(tick, group):
        return whole(xin[tick, 2 * is_first if group == 0 else 1])

    def cot_block(tick, group):
        return whole(cot[tick, 0 if group == 0 else 1 + is_last])

    def norm_parts(values, group):
        inv_root = lax.rsqrt(jnp.mean(values * values, axis=-1, keepdims=True) + epsilon)
        scaled = values * inv_root
        return scaled, inv_root, (scaled * gain_ref[pl.ds(group, 1), :]).astype(jnp.bfloat16)

    def value_product(rows_of, group):
        return contract_sum(
            width,
            lambda at: jnp.dot(rows_of(at), wv[group, at, :], preferred_element_type=jnp.float32),
            (rows, features),
        ).astype(jnp.bfloat16)

    def arrive(tick, stream):
        @pl.when(tick > 0)
        def _():
            shift_arrival(tick, stream).wait_recv()

    def weights_ready(tick, index):
        @pl.when(tick == 0)
        def _():
            weight_copies[index].wait()

    def forward_start(tick, group):
        arrive(tick, group)
        lhs[...] = norm_parts(input_block(tick, group), group)[2]
        weights_ready(tick, 2 * group)
        values = value_product(lambda at: lhs[:, at], group)
        weights_ready(tick, 2 * group + 1)

        def step(at):
            psend[tick, group, :, at] = jnp.dot(
                values, wo[group, :, at], preferred_element_type=jnp.float32
            ).astype(jnp.bfloat16)

        chunk_loop(width, step)
        exchange(tick, group).start()

    def send_on(tick, stream):
        @pl.when(tick < ticks - 1)
        def _():
            shift(tick, stream).start()

    def peer_sum(tick, stream):
        exchange(tick, stream).wait_recv()
        return psend[tick, stream].astype(jnp.float32) + precv[tick, stream].astype(jnp.float32)

    def forward_finish(tick, group):
        outputs = parted(input_block(tick, group) + peer_sum(tick, group))
        moved[tick, group] = outputs
        send_on(tick, group)
        if group == 1:
            @pl.when((tick < ticks - 1) & (s == sections - 1))
            def _():
                cot[tick + 1, 2] = (
                    outputs.astype(jnp.float32) - tgt[tick].astype(jnp.float32)
                ).astype(jnp.bfloat16)

    def backward_start(tick, group):
        arrive(tick, 2 + group)
        up_ref[group, tick] = cot_block(tick, group).astype(jnp.bfloat16)
        down = contract_sum(
            width,
            lambda at: times_transposed(up_ref[group, tick, :, at], wo[group, :, at]),
            (rows, features),
        ).astype(jnp.bfloat16)
        down_ref[group, tick] = down

        def step(at):
            psend[tick, 2 + group, :, at] = times_transposed(down, wv[group, at, :]).astype(
                jnp.bfloat16
            )

        chunk_loop(width, step)
        exchange(tick, 2 + group).start()

    def stash_step(tick, group):
        block = xin[tick, 2 * is_first if group == 0 else 1]
        for slot in range(slots):
            stash[slot, group] = jnp.where(fill_ref[group, tick] == slot, block, stash[slot, group])

    def source_values(tick, group):
        normed_ref[group, tick] = norm_parts(whole(stash[read_ref[group, tick], group]), group)[2]
        vals_ref[group, tick] = value_product(lambda at: normed_ref[group, tick, :, at], group)

    def backward_finish(tick, group):
        scaled, inv_root, _ = norm_parts(whole(stash[read_ref[group, tick], group]), group)
        pulled = peer_sum(tick, 2 + group)
        weighted = pulled * gain_ref[pl.ds(group, 1), :]
        inner_mean = jnp.mean(weighted * scaled, axis=-1, keepdims=True)
        moved[tick, 2 + group] = parted(
            cot_block(tick, group) + inv_root * (weighted - scaled * inner_mean)
        )
        send_on(tick, 2 + group)
        gain_out_ref[pl.ds(group, 1), :] += jnp.sum(pulled * scaled, axis=0, keepdims=True)

    first_in.wait_recv()
    xin[0, 2] = xin[0, 0]

    @pl.when(s == 0)
    def _():
        fresh_copy.wait()

    @pl.when(s == sections - 1)
    def _():
        target_copy.wait()

    def tick_step(tick, _):
        forward_start(tick, 0)
        forward_start(tick, 1)
        forward_finish(tick, 0)

        @pl.when(tick == 0)
        def _():
            first_cot.wait_recv()
            cot[0, 2] = cot[0, 1]

        backward_start(tick, 0)
        forward_finish(tick, 1)

        @pl.when(tick == 0)
        def _():
            first_stash.wait_recv()

        stash_step(tick, 0)
        stash_step(tick, 1)
        backward_start(tick, 1)
        backward_finish(tick, 0)
        source_values(tick, 0)
        source_values(tick, 1)
        backward_finish(tick, 1)
        return None

    lax.fori_loop(0, ticks, tick_step, None)

    for group in range(2):
        activ_ref[group] = moved[ticks - 1, group, d]
        cotan_ref[group] = moved[ticks - 1, 2 + group, d]
        for slot in range(slots):
            stash_out_ref[slot, group] = stash[slot, group, d]
    gain_out_ref[...] = gain_out_ref[...] * (ticks * rows) ** (-0.5)
    for copy in (first_in, first_cot, first_stash):
        copy.wait_send()
    for tick in range(ticks):
        for stream in range(4):
            exchange(tick, stream).wait_send()
            if tick < ticks - 1:
                shift(tick, stream).wait_send()


def grads_kernel(
    grad_scale, activ_ref, cotan_ref, stash_ref, gain_ref, normed_ref, down_ref, vals_ref, up_ref,
    activ_hbm, cotan_hbm, stash_hbm, value_hbm, out_hbm, gain_hbm,
    value_grad, out_grad, small_sem, grad_sem,
):
    small = [
        pltpu.make_async_copy(source, target, small_sem.at[index])
        for index, (source, target) in enumerate(
            ((activ_ref, activ_hbm), (cotan_ref, cotan_hbm), (stash_ref, stash_hbm), (gain_ref, gain_hbm))
        )
    ]
    for copy in small:
        copy.start()
    width = normed_ref.shape[2]
    size = CHUNK if width % CHUNK == 0 else width

    def step(index, _):
        at = pl.ds(pl.multiple_of(index * size, size), size)
        for group in range(2):
            value_grad[group, at, :] = (
                transposed_times(normed_ref[group, :, at], down_ref[group]) * grad_scale
            ).astype(jnp.bfloat16)
            pltpu.make_async_copy(
                value_grad.at[group, at, :], value_hbm.at[group, at, :], grad_sem.at[0]
            ).start()
            out_grad[group, :, at] = (
                transposed_times(vals_ref[group], up_ref[group, :, at]) * grad_scale
            ).astype(jnp.bfloat16)
            pltpu.make_async_copy(
                out_grad.at[group, :, at], out_hbm.at[group, :, at], grad_sem.at[1]
            ).start()
        return None

    lax.fori_loop(0, width // size, step, None)
    pltpu.make_async_copy(value_grad, value_hbm, grad_sem.at[0]).wait()
    pltpu.make_async_copy(out_grad, out_hbm, grad_sem.at[1]).wait()
    for copy in small:
        copy.wait()


def relay_body(
    sections,
    w_value,
    w_out,
    norm_gain,
    saved_inputs,
    arriving,
    returning,
    fresh_rows,
    targets,
    fill_slots,
    read_slots,
):
    value_mats, out_mats, gains = w_value[0], w_out[0], norm_gain[0]
    saved, activations, cotangents = saved_inputs[0], arriving[0], returning[0]
    ticks, half, width = fresh_rows.shape
    features = value_mats.shape[2]
    slots = saved.shape[0]
    rows = 2 * half
    vmem = pl.BlockSpec(memory_space=pltpu.VMEM)
    smem = pl.BlockSpec(memory_space=pltpu.SMEM)
    hbm = pl.BlockSpec(memory_space=pl.ANY)
    shape = jax.ShapeDtypeStruct
    narrow = jnp.bfloat16
    final_rows, gradients, stash_rows, normed, down, values, upstream, gain_sums = pl.pallas_call(
        functools.partial(relay_kernel, sections),
        out_shape=(
            shape(activations.shape, narrow),
            shape(cotangents.shape, narrow),
            shape(saved.shape, narrow),
            shape((2, ticks, rows, width), narrow),
            shape((2, ticks, rows, features), narrow),
            shape((2, ticks, rows, features), narrow),
            shape((2, ticks, rows, width), narrow),
            shape(gains.shape, jnp.float32),
        ),
        in_specs=[hbm, hbm] + [vmem] * 6 + [smem] * 2,
        out_specs=(vmem,) * 8,
        scratch_shapes=[
            pltpu.VMEM(value_mats.shape, narrow),
            pltpu.VMEM(out_mats.shape, narrow),
            pltpu.VMEM((ticks, 3, 2, half, width), narrow),
            pltpu.VMEM((ticks, 3, 2, half, width), narrow),
            pltpu.VMEM((slots, 2, 2, half, width), narrow),
            pltpu.VMEM((ticks, 2, half, width), narrow),
            pltpu.VMEM((ticks, 4, rows, width), narrow),
            pltpu.VMEM((ticks, 4, rows, width), narrow),
            pltpu.VMEM((ticks, 4, 2, half, width), narrow),
            pltpu.VMEM((rows, width), narrow),
            pltpu.SemaphoreType.DMA((2, 2)),
            pltpu.SemaphoreType.DMA((5,)),
            pltpu.SemaphoreType.DMA((5,)),
            pltpu.SemaphoreType.DMA((ticks, 4)),
            pltpu.SemaphoreType.DMA((ticks, 4)),
            pltpu.SemaphoreType.DMA((ticks, 4)),
            pltpu.SemaphoreType.DMA((ticks, 4)),
        ],
        compiler_params=pltpu.CompilerParams(
            collective_id=0, has_side_effects=True, vmem_limit_bytes=VMEM_GRANT
        ),
    )(
        value_mats, out_mats, gains, saved, activations, cotangents,
        fresh_rows, targets, fill_slots[0].T, read_slots[0].T,
    )
    flat = lambda block: block.reshape(2, ticks * rows, block.shape[3])
    grads = pl.pallas_call(
        functools.partial(grads_kernel, (ticks * rows) ** (-0.5)),
        out_shape=(
            shape(activations.shape, narrow),
            shape(cotangents.shape, narrow),
            shape(saved.shape, narrow),
            shape(value_mats.shape, narrow),
            shape(out_mats.shape, narrow),
            shape(gains.shape, jnp.float32),
        ),
        in_specs=[vmem] * 8,
        out_specs=(hbm,) * 6,
        scratch_shapes=[
            pltpu.VMEM(value_mats.shape, narrow),
            pltpu.VMEM(out_mats.shape, narrow),
            pltpu.SemaphoreType.DMA((4,)),
            pltpu.SemaphoreType.DMA((2,)),
        ],
        compiler_params=pltpu.CompilerParams(vmem_limit_bytes=VMEM_GRANT),
    )(final_rows, gradients, stash_rows, gain_sums, flat(normed), flat(down), flat(values), flat(upstream))
    return tuple(block[None] for block in grads)


def solution(mesh):
    in_specs = (
        P("section", None, None, "dp"),
        P("section", None, "dp", None),
        P("section", None, None),
        P("section", None, None, "dp", None),
        P("section", None, "dp", None),
        P("section", None, "dp", None),
        P(None, "dp", None),
        P(None, "dp", None),
        P("section", None, None),
        P("section", None, None),
    )
    out_specs = (
        P("section", None, "dp", None),
        P("section", None, "dp", None),
        P("section", None, None, "dp", None),
        P("section", None, None, "dp"),
        P("section", None, "dp", None),
        P("section", None, None),
    )
    paired = mesh.shape["dp"] == 2 and mesh.shape["section"] > 2
    program = functools.partial(relay_body, mesh.shape["section"]) if paired else body
    return jax.shard_map(program, mesh=mesh, in_specs=in_specs, out_specs=out_specs, check_vma=False)
```

```python
import functools

import jax
import jax.numpy as jnp
from jax import lax
from jax.experimental import pallas as pl
from jax.experimental.pallas import tpu as pltpu
from jax.sharding import PartitionSpec as P

epsilon = 1e-06


def shifted(shard, axis, by):
    devices = lax.axis_size(axis)
    return lax.ppermute(shard, axis, [(i, (i + by) % devices) for i in range(devices)])


def normalize(block_rows, gain_row):
    values = block_rows.astype(jnp.float32)
    inv_root = lax.rsqrt(jnp.mean(values * values, axis=-1, keepdims=True) + epsilon)
    scaled = values * inv_root
    return (scaled, inv_root, (scaled * gain_row).astype(jnp.bfloat16))


def times_transposed(left, right):
    return lax.dot_general(
        left, right, (((1,), (1,)), ((), ())), preferred_element_type=jnp.float32
    )


def transposed_times(left, right):
    return lax.dot_general(
        left, right, (((0,), (0,)), ((), ())), preferred_element_type=jnp.float32
    )


def weight_terms(value_group, normed_all, down_grad, upstream_all):
    values = jnp.dot(normed_all, value_group, preferred_element_type=jnp.float32).astype(
        jnp.bfloat16
    )
    return (transposed_times(normed_all, down_grad), transposed_times(values, upstream_all))


def body(
    w_value,
    w_out,
    norm_gain,
    saved_inputs,
    arriving,
    returning,
    fresh_rows,
    targets,
    fill_slots,
    read_slots,
):
    value_mats = w_value[0]
    out_mats = w_out[0]
    gains = norm_gain[0]
    saved = saved_inputs[0]
    activations = arriving[0]
    cotangents = returning[0]
    tick_count = fresh_rows.shape[0]
    tok_rows = activations.shape[1]
    all_rows = tok_rows * lax.axis_size("dp")
    section_index = lax.axis_index("section")
    last_section = lax.axis_size("section") - 1
    row_offset = lax.axis_index("dp") * tok_rows
    activations, new_rows = (
        lax.all_gather(activations, "dp", axis=1, tiled=True),
        lax.all_gather(fresh_rows, "dp", axis=1, tiled=True),
    )

    def own_rows(block):
        return lax.dynamic_slice_in_dim(block, row_offset, tok_rows, 0)

    def forward(block, group):
        scaled, inv_root, normed = normalize(block, gains[group])
        values = jnp.dot(normed, value_mats[group], preferred_element_type=jnp.float32).astype(
            jnp.bfloat16
        )
        summed = lax.psum(
            jnp.dot(values, out_mats[group], preferred_element_type=jnp.float32).astype(
                jnp.bfloat16
            ),
            "dp",
        ).astype(jnp.float32)
        return (block.astype(jnp.float32) + summed).astype(jnp.bfloat16)

    value_sums = [jnp.zeros(value_mats.shape[1:], jnp.float32) for group in range(2)]
    out_sums = [jnp.zeros(out_mats.shape[1:], jnp.float32) for group in range(2)]
    gain_sums = [jnp.zeros(gains.shape[1:], jnp.float32) for group in range(2)]
    outputs = activations
    gradients = cotangents
    for tick_index in range(tick_count):
        if tick_index > 0:
            received = shifted(outputs, "section", 1)
            lower_group = jnp.where(section_index == 0, new_rows[tick_index], received[0])
            upper_group = jnp.where(section_index == 0, received[0], received[1])
            activations = jnp.stack([lower_group, upper_group])
            returned = shifted(gradients, "section", -1)
            finish = (
                own_rows(outputs[1]).astype(jnp.float32)
                - targets[tick_index - 1].astype(jnp.float32)
            ).astype(jnp.bfloat16)
            cotangents = jnp.stack(
                [
                    jnp.where(section_index == last_section, returned[1], returned[0]),
                    jnp.where(section_index == last_section, finish, returned[1]),
                ]
            )
        for group in range(2):
            saved = saved.at[fill_slots[0, tick_index, group], group].set(
                own_rows(activations[group])
            )
        outputs = jnp.stack([forward(activations[0], 0), forward(activations[1], 1)])
        fresh_grads = []
        for group in range(2):
            source = saved[read_slots[0, tick_index, group], group]
            scaled, inv_root, normed = normalize(source, gains[group])
            normed_all, upstream_all = (
                lax.all_gather(normed, "dp", axis=0, tiled=True),
                lax.all_gather(cotangents[group], "dp", axis=0, tiled=True),
            )
            down_grad = times_transposed(upstream_all, out_mats[group]).astype(jnp.bfloat16)
            pulled = lax.psum_scatter(
                times_transposed(down_grad, value_mats[group]).astype(jnp.bfloat16),
                "dp",
                scatter_dimension=0,
                tiled=True,
            ).astype(jnp.float32)
            weighted = pulled * gains[group]
            inner_mean = jnp.mean(weighted * scaled, axis=-1, keepdims=True)
            fresh_grads.append(
                (
                    cotangents[group].astype(jnp.float32)
                    + inv_root * (weighted - scaled * inner_mean)
                ).astype(jnp.bfloat16)
            )
            gain_sums[group] = gain_sums[group] + jnp.sum(pulled * scaled, axis=0)
            value_term, out_term = weight_terms(
                value_mats[group], normed_all, down_grad, upstream_all
            )
            value_sums[group] = value_sums[group] + value_term
            out_sums[group] = out_sums[group] + out_term
        gradients = jnp.stack(fresh_grads)
    grad_scale = (tick_count * all_rows) ** (-0.5)
    gain_total = lax.psum(jnp.stack(gain_sums).astype(jnp.bfloat16), "dp").astype(jnp.float32)
    final_rows = jnp.stack([own_rows(outputs[0]), own_rows(outputs[1])])
    return (
        final_rows[None],
        gradients[None],
        saved[None],
        (jnp.stack(value_sums) * grad_scale).astype(jnp.bfloat16)[None],
        (jnp.stack(out_sums) * grad_scale).astype(jnp.bfloat16)[None],
        (gain_total * grad_scale)[None],
    )


CHUNK = 512
VMEM_GRANT = 60 * 1024 * 1024
MESH = pl.DeviceIdType.MESH


def chunk_loop(width, step):
    size = CHUNK if width % CHUNK == 0 else width
    lax.fori_loop(0, width // size, lambda i, _: step(pl.ds(pl.multiple_of(i * size, size), size)), None, unroll=UNROLL)


UNROLL = 9


def contract_sum(width, term, shape):
    size = CHUNK if width % CHUNK == 0 else width

    def step(i, total):
        return total + term(pl.ds(pl.multiple_of(i * size, size), size))

    return lax.fori_loop(0, width // size, step, jnp.zeros(shape, jnp.float32), unroll=UNROLL)


def relay_kernel(
    sections,
    wv_hbm,
    wo_hbm,
    gain_ref,
    saved_ref,
    arriving_ref,
    returning_ref,
    fresh_ref,
    targets_ref,
    fill_ref,
    read_ref,
    activ_ref,
    cotan_ref,
    stash_ref,
    normed_ref,
    down_ref,
    vals_ref,
    up_ref,
    gain_out_ref,
    wv,
    wo,
    xin,
    cot,
    staged,
    landed,
    peer_stash,
    psend,
    precv,
    moved,
    lhs,
    scaled_own,
    root_own,
    gain_sum,
    gain_send,
    gain_recv,
    w_sem,
    ex_send,
    ex_recv,
    sh_send,
    sh_recv,
    st_send,
    st_recv,
    side_send,
    side_recv,
):
    s = lax.axis_index("section")
    d = lax.axis_index("dp")
    peer = 1 - d
    after = lax.rem(s + 1, sections)
    before = lax.rem(s + sections - 1, sections)
    is_last = s // (sections - 1)
    is_first = before // (sections - 1)
    ticks = fresh_ref.shape[0]
    half, width = arriving_ref.shape[1:]
    rows = 2 * half
    features = wv.shape[2]
    slots = saved_ref.shape[0]

    weight_copies = {}
    for group in range(2):
        for index, (source, target) in enumerate(((wv_hbm, wv), (wo_hbm, wo))):
            weight_copies[group, index] = pltpu.make_async_copy(
                source.at[group], target.at[group], w_sem.at[group, index]
            )
    for key in ((0, 0), (0, 1), (1, 1), (1, 0)):
        weight_copies[key].start()

    barrier = pltpu.get_barrier_semaphore()
    for target in ((s, peer), (after, d), (before, d), (after, peer), (before, peer)):
        pl.semaphore_signal(barrier, inc=1, device_id=target, device_id_type=MESH)

    for group in range(2):
        xin[0, group, 0] = arriving_ref[group]
        cot[0, group, 0] = returning_ref[group]
    for tick in range(1, ticks):
        xin[tick, 2, 0] = fresh_ref[tick]
    for group in range(2):
        for index in range(slots - 1):
            staged[index, group] = jnp.where(
                fill_ref[group, 0] <= index, saved_ref[index + 1, group], saved_ref[index, group]
            )
    stash_ref[...] = saved_ref[...]
    gain_sum[...] = jnp.zeros_like(gain_sum)
    pl.semaphore_wait(barrier, 5)

    def remote(src, dst, send, recv, target):
        return pltpu.make_async_remote_copy(
            src_ref=src, dst_ref=dst, send_sem=send, recv_sem=recv,
            device_id=target, device_id_type=MESH,
        )

    def initial(stream):
        group = stream % 2
        source, buffer = (arriving_ref, xin) if stream < 2 else (returning_ref, cot)
        return remote(
            source.at[group], buffer.at[0, group, 1],
            sh_send.at[0, stream, 1], sh_recv.at[0, stream, 1], (s, peer),
        )

    def stash_copy(index, group):
        return remote(
            staged.at[index, group], landed.at[index, group],
            st_send.at[index, group], st_recv.at[index, group], (s, peer),
        )

    fresh_copy = remote(
        fresh_ref.at[pl.ds(1, ticks - 1)], xin.at[pl.ds(1, ticks - 1), 2, 1],
        side_send.at[0], side_recv.at[0], (s, peer),
    )
    gain_copy = remote(gain_send, gain_recv, side_send.at[1], side_recv.at[1], (s, peer))
    for stream in (0, 3, 1, 2):
        initial(stream).start()

    def whole(block):
        return block.astype(jnp.float32).reshape(rows, block.shape[2])

    def parted(block):
        return block.reshape(2, half, block.shape[1]).astype(jnp.bfloat16)

    def exchange(tick, stream):
        return remote(
            psend.at[tick, stream, 1], precv.at[tick, stream],
            ex_send.at[tick, stream], ex_recv.at[tick, stream], (s, peer),
        )

    def shift(tick, stream, side):
        group = stream % 2
        if stream < 2:
            place, target, buffer = (group + is_last) % 2, after, xin
        else:
            place, target, buffer = (group + is_first) % 2, before, cot
        return remote(
            moved.at[tick, stream], buffer.at[tick + 1, place, side],
            sh_send.at[tick + 1, stream, side], sh_recv.at[tick + 1, stream - group + place, side],
            (target, peer if side else d),
        )

    def finish_copy(tick):
        return remote(
            cot.at[tick + 1, 1, 0], cot.at[tick + 1, 1, 1],
            sh_send.at[tick + 1, 1, 1], sh_recv.at[tick + 1, 3, 1], (s, peer),
        )

    def arrival(tick, stream, side):
        buffer = xin if stream < 2 else cot
        return remote(
            moved.at[0, stream], buffer.at[tick, stream % 2, side],
            sh_send.at[tick, stream, side], sh_recv.at[tick, stream, side], (s, peer),
        )

    def arrive(tick, stream):
        later = tick > 0
        if stream == 0:
            near, far = later & (s != 0), (tick == 0) | (s != 0)
        elif stream == 3:
            near, far = later & (s != sections - 1), None
        else:
            near, far = later, None

        @pl.when(near)
        def _():
            arrival(tick, stream, 0).wait_recv()

        if far is None:
            arrival(tick, stream, 1).wait_recv()
        else:
            @pl.when(far)
            def _():
                arrival(tick, stream, 1).wait_recv()

            @pl.when((tick == 1) & (s == 0))
            def _():
                fresh_copy.wait_recv()

    def input_place(tick, group):
        return 2 * is_first * jnp.minimum(tick, 1) if group == 0 else 1

    def norm_parts(values, group):
        inv_root = lax.rsqrt(jnp.mean(values * values, axis=-1, keepdims=True) + epsilon)
        scaled = values * inv_root
        return scaled, inv_root, (scaled * gain_ref[pl.ds(group, 1), :]).astype(jnp.bfloat16)

    def weights_ready(tick, key):
        @pl.when(tick == 0)
        def _():
            weight_copies[key].wait()

    def side_sends(tick, stream):
        group, index = stream % 2, stream // 2

        @pl.when(tick == 0)
        def _():
            for part in range(index, slots - 1, 2):
                stash_copy(part, group).start()

        if stream == 3:
            @pl.when((tick == 0) & (s == 0))
            def _():
                fresh_copy.start()

    def forward_start(tick, group):
        arrive(tick, group)
        lhs[...] = norm_parts(whole(xin[tick, input_place(tick, group)]), group)[2]
        if group == 0:
            weights_ready(tick, (0, 0))
        values = contract_sum(
            width,
            lambda at: jnp.dot(lhs[:, at], wv[group, at, :], preferred_element_type=jnp.float32),
            (rows, features),
        ).astype(jnp.bfloat16)
        if group == 0:
            weights_ready(tick, (0, 1))

        def step(at):
            psend[tick, group, :, :, at] = parted(
                jnp.dot(values, wo[group, :, at], preferred_element_type=jnp.float32)
            )

        chunk_loop(width, step)
        exchange(tick, group).start()
        side_sends(tick, group)

    def peer_sum(tick, stream):
        exchange(tick, stream).wait_recv()
        return psend[tick, stream, 0].astype(jnp.float32) + precv[tick, stream].astype(jnp.float32)

    def forward_finish(tick, group):
        own = xin[tick, input_place(tick, group), 0].astype(jnp.float32)
        outputs = (own + peer_sum(tick, group)).astype(jnp.bfloat16)
        moved[tick, group] = outputs
        going = tick < ticks - 1

        @pl.when(going if group == 0 else going & (s != sections - 1))
        def _():
            shift(tick, group, 1).start()
            shift(tick, group, 0).start()

        if group == 1:
            @pl.when(going & (s == sections - 1))
            def _():
                cot[tick + 1, 1, 0] = (
                    outputs.astype(jnp.float32) - targets_ref[tick].astype(jnp.float32)
                ).astype(jnp.bfloat16)
                finish_copy(tick).start()

    def backward_start(tick, group):
        arrive(tick, 2 + group)
        up_ref[group, tick] = whole(cot[tick, group]).astype(jnp.bfloat16)
        if group == 1:
            weights_ready(tick, (1, 1))
        down = contract_sum(
            width,
            lambda at: times_transposed(up_ref[group, tick, :, at], wo[group, :, at]),
            (rows, features),
        ).astype(jnp.bfloat16)
        down_ref[group, tick] = down
        if group == 1:
            weights_ready(tick, (1, 0))

        def step(at):
            psend[tick, 2 + group, :, :, at] = parted(times_transposed(down, wv[group, at, :]))

        chunk_loop(width, step)
        exchange(tick, 2 + group).start()
        side_sends(tick, 2 + group)

    def own_source(tick, group):
        block = xin[tick, input_place(tick, group), 0]
        for slot in range(slots):
            stash_ref[slot, group] = jnp.where(fill_ref[group, tick] == slot, block, stash_ref[slot, group])
        source = stash_ref[read_ref[group, tick], group].astype(jnp.float32)
        scaled, inv_root, normed = norm_parts(source, group)
        normed_ref[group, tick, 0] = normed
        scaled_own[group] = scaled
        root_own[group] = jnp.broadcast_to(inv_root, root_own.shape[1:])
        gain_sum[group] += psend[tick, 2 + group, 0].astype(jnp.float32) * scaled

    def peer_source(tick, group):
        @pl.when(tick == 0)
        def _():
            filled = fill_ref[group, 0]
            for index in range(slots - 1):
                stash_copy(index, group).wait_recv()
            for slot in range(slots):
                low, high = max(slot - 1, 0), min(slot, slots - 2)
                peer_stash[slot, group] = jnp.where(filled < slot, landed[low, group], landed[high, group])

        block = xin[tick, input_place(tick, group), 1]
        for slot in range(slots):
            peer_stash[slot, group] = jnp.where(
                fill_ref[group, tick] == slot, block, peer_stash[slot, group]
            )
        source = peer_stash[read_ref[group, tick], group].astype(jnp.float32)
        scaled, _, normed = norm_parts(source, group)
        normed_ref[group, tick, 1] = normed
        gain_sum[group] += psend[tick, 2 + group, 1].astype(jnp.float32) * scaled

    def backward_finish(tick, group):
        scaled = scaled_own[group]
        pulled = peer_sum(tick, 2 + group)
        weighted = pulled * gain_ref[pl.ds(group, 1), :]
        inner_mean = jnp.mean(weighted * scaled, axis=-1, keepdims=True)
        moved[tick, 2 + group] = (
            cot[tick, group, 0].astype(jnp.float32)
            + root_own[group][:, :1] * (weighted - scaled * inner_mean)
        ).astype(jnp.bfloat16)
        going = tick < ticks - 1

        @pl.when(going if group == 1 else going & (s != 0))
        def _():
            shift(tick, 2 + group, 1).start()
            shift(tick, 2 + group, 0).start()

    def tick_step(tick, _):
        forward_start(tick, 0)
        backward_start(tick, 1)

        @pl.when(tick > 0)
        def _():
            backward_finish(tick - 1, 0)
            peer_source(tick - 1, 1)

        forward_finish(tick, 0)
        forward_start(tick, 1)

        @pl.when(tick > 0)
        def _():
            peer_source(tick - 1, 0)

        own_source(tick, 1)
        backward_finish(tick, 1)
        backward_start(tick, 0)
        own_source(tick, 0)
        forward_finish(tick, 1)
        return None

    lax.fori_loop(0, ticks, tick_step, None)

    for group in (1, 0):
        peer_source(ticks - 1, group)
        gain_send[pl.ds(group, 1), :] = jnp.sum(gain_sum[group], axis=0, keepdims=True)
    gain_copy.start()
    for group in range(2):
        def chunk_values(at):
            block = normed_ref[group, :, :, :, at].astype(jnp.float32)
            left = block.reshape(ticks * rows, block.shape[3]).astype(jnp.bfloat16)
            return jnp.dot(left, wv[group, at, :], preferred_element_type=jnp.float32)

        vals_ref[group] = contract_sum(width, chunk_values, (ticks * rows, features)).astype(jnp.bfloat16)
    backward_finish(ticks - 1, 0)
    for group in range(2):
        activ_ref[group] = moved[ticks - 1, group]
        cotan_ref[group] = moved[ticks - 1, 2 + group]
    gain_copy.wait()
    gain_out_ref[...] = (gain_send[...] + gain_recv[...]) * (ticks * rows) ** (-0.5)

    for stream in range(4):
        initial(stream).wait_send()
    for group in range(2):
        for index in range(slots - 1):
            stash_copy(index, group).wait_send()

    @pl.when(s == 0)
    def _():
        fresh_copy.wait_send()

    for tick in range(ticks):
        for stream in range(4):
            exchange(tick, stream).wait_send()
    for tick in range(ticks - 1):
        for side in range(2):
            shift(tick, 0, side).wait_send()
            shift(tick, 3, side).wait_send()

        @pl.when(s != sections - 1)
        def _():
            for side in range(2):
                shift(tick, 1, side).wait_send()

        @pl.when(s == sections - 1)
        def _():
            finish_copy(tick).wait_send()

        @pl.when(s != 0)
        def _():
            for side in range(2):
                shift(tick, 2, side).wait_send()


def grads_kernel(
    grad_scale, activ_ref, cotan_ref, stash_ref, gain_ref, normed_ref, down_ref, vals_ref, up_ref,
    activ_hbm, cotan_hbm, stash_hbm, value_hbm, out_hbm, gain_hbm,
    value_grad, out_grad, small_sem, grad_sem,
):
    small = [
        pltpu.make_async_copy(source, target, small_sem.at[index])
        for index, (source, target) in enumerate(
            ((activ_ref, activ_hbm), (cotan_ref, cotan_hbm), (stash_ref, stash_hbm), (gain_ref, gain_hbm))
        )
    ]
    for copy in small:
        copy.start()
    width = normed_ref.shape[2]
    size = CHUNK if width % CHUNK == 0 else width

    def step(index, _):
        at = pl.ds(pl.multiple_of(index * size, size), size)
        for group in range(2):
            value_grad[group, at, :] = (
                transposed_times(normed_ref[group, :, at], down_ref[group]) * grad_scale
            ).astype(jnp.bfloat16)
            pltpu.make_async_copy(
                value_grad.at[group, at, :], value_hbm.at[group, at, :], grad_sem.at[0]
            ).start()
            out_grad[group, :, at] = (
                transposed_times(vals_ref[group], up_ref[group, :, at]) * grad_scale
            ).astype(jnp.bfloat16)
            pltpu.make_async_copy(
                out_grad.at[group, :, at], out_hbm.at[group, :, at], grad_sem.at[1]
            ).start()
        return None

    lax.fori_loop(0, width // size, step, None)
    pltpu.make_async_copy(value_grad, value_hbm, grad_sem.at[0]).wait()
    pltpu.make_async_copy(out_grad, out_hbm, grad_sem.at[1]).wait()
    for copy in small:
        copy.wait()


def relay_body(
    sections,
    w_value,
    w_out,
    norm_gain,
    saved_inputs,
    arriving,
    returning,
    fresh_rows,
    targets,
    fill_slots,
    read_slots,
):
    value_mats, out_mats, gains = w_value[0], w_out[0], norm_gain[0]
    saved, activations, cotangents = saved_inputs[0], arriving[0], returning[0]
    ticks, half, width = fresh_rows.shape
    features = value_mats.shape[2]
    slots = saved.shape[0]
    if slots < 2:
        return body(
            w_value, w_out, norm_gain, saved_inputs, arriving,
            returning, fresh_rows, targets, fill_slots, read_slots,
        )
    rows = 2 * half
    vmem = pl.BlockSpec(memory_space=pltpu.VMEM)
    smem = pl.BlockSpec(memory_space=pltpu.SMEM)
    hbm = pl.BlockSpec(memory_space=pl.ANY)
    shape = jax.ShapeDtypeStruct
    narrow = jnp.bfloat16
    final_rows, gradients, stash_rows, normed, down, values, upstream, gain_sums = pl.pallas_call(
        functools.partial(relay_kernel, sections),
        out_shape=(
            shape(activations.shape, narrow),
            shape(cotangents.shape, narrow),
            shape(saved.shape, narrow),
            shape((2, ticks, 2, half, width), narrow),
            shape((2, ticks, rows, features), narrow),
            shape((2, ticks * rows, features), narrow),
            shape((2, ticks, rows, width), narrow),
            shape(gains.shape, jnp.float32),
        ),
        in_specs=[hbm, hbm] + [vmem] * 6 + [smem] * 2,
        out_specs=(vmem,) * 8,
        scratch_shapes=[
            pltpu.VMEM(value_mats.shape, narrow),
            pltpu.VMEM(out_mats.shape, narrow),
            pltpu.VMEM((ticks, 3, 2, half, width), narrow),
            pltpu.VMEM((ticks, 2, 2, half, width), narrow),
            pltpu.VMEM((slots - 1, 2, half, width), narrow),
            pltpu.VMEM((slots - 1, 2, half, width), narrow),
            pltpu.VMEM((slots, 2, half, width), narrow),
            pltpu.VMEM((ticks, 4, 2, half, width), narrow),
            pltpu.VMEM((ticks, 4, half, width), narrow),
            pltpu.VMEM((ticks, 4, half, width), narrow),
            pltpu.VMEM((rows, width), narrow),
            pltpu.VMEM((2, half, width), jnp.float32),
            pltpu.VMEM((2, half, 128), jnp.float32),
            pltpu.VMEM((2, half, width), jnp.float32),
            pltpu.VMEM((2, width), jnp.float32),
            pltpu.VMEM((2, width), jnp.float32),
            pltpu.SemaphoreType.DMA((2, 2)),
            pltpu.SemaphoreType.DMA((ticks, 4)),
            pltpu.SemaphoreType.DMA((ticks, 4)),
            pltpu.SemaphoreType.DMA((ticks, 4, 2)),
            pltpu.SemaphoreType.DMA((ticks, 4, 2)),
            pltpu.SemaphoreType.DMA((slots - 1, 2)),
            pltpu.SemaphoreType.DMA((slots - 1, 2)),
            pltpu.SemaphoreType.DMA((2,)),
            pltpu.SemaphoreType.DMA((2,)),
        ],
        compiler_params=pltpu.CompilerParams(
            collective_id=0, has_side_effects=True, vmem_limit_bytes=VMEM_GRANT
        ),
    )(
        value_mats, out_mats, gains, saved, activations, cotangents,
        fresh_rows, targets, fill_slots[0].T, read_slots[0].T,
    )
    flat = lambda block: block.reshape(2, ticks * rows, block.shape[-1])
    grads = pl.pallas_call(
        functools.partial(grads_kernel, (ticks * rows) ** (-0.5)),
        out_shape=(
            shape(activations.shape, narrow),
            shape(cotangents.shape, narrow),
            shape(saved.shape, narrow),
            shape(value_mats.shape, narrow),
            shape(out_mats.shape, narrow),
            shape(gains.shape, jnp.float32),
        ),
        in_specs=[vmem] * 8,
        out_specs=(hbm,) * 6,
        scratch_shapes=[
            pltpu.VMEM(value_mats.shape, narrow),
            pltpu.VMEM(out_mats.shape, narrow),
            pltpu.SemaphoreType.DMA((4,)),
            pltpu.SemaphoreType.DMA((2,)),
        ],
        compiler_params=pltpu.CompilerParams(vmem_limit_bytes=VMEM_GRANT),
    )(final_rows, gradients, stash_rows, gain_sums, flat(normed), flat(down), flat(values), flat(upstream))
    return tuple(block[None] for block in grads)


def solution(mesh):
    in_specs = (
        P("section", None, None, "dp"),
        P("section", None, "dp", None),
        P("section", None, None),
        P("section", None, None, "dp", None),
        P("section", None, "dp", None),
        P("section", None, "dp", None),
        P(None, "dp", None),
        P(None, "dp", None),
        P("section", None, None),
        P("section", None, None),
    )
    out_specs = (
        P("section", None, "dp", None),
        P("section", None, "dp", None),
        P("section", None, None, "dp", None),
        P("section", None, None, "dp"),
        P("section", None, "dp", None),
        P("section", None, None),
    )
    paired = mesh.shape["dp"] == 2 and mesh.shape["section"] > 2
    program = functools.partial(relay_body, mesh.shape["section"]) if paired else body
    return jax.shard_map(program, mesh=mesh, in_specs=in_specs, out_specs=out_specs, check_vma=False)
```

```python
import functools

import jax
import jax.numpy as jnp
from jax import lax
from jax.experimental import pallas as pl
from jax.experimental.pallas import tpu as pltpu
from jax.sharding import PartitionSpec as P

epsilon = 1e-06


def shifted(shard, axis, by):
    devices = lax.axis_size(axis)
    return lax.ppermute(shard, axis, [(i, (i + by) % devices) for i in range(devices)])


def normalize(block_rows, gain_row):
    values = block_rows.astype(jnp.float32)
    inv_root = lax.rsqrt(jnp.mean(values * values, axis=-1, keepdims=True) + epsilon)
    scaled = values * inv_root
    return (scaled, inv_root, (scaled * gain_row).astype(jnp.bfloat16))


def times_transposed(left, right):
    return lax.dot_general(
        left, right, (((1,), (1,)), ((), ())), preferred_element_type=jnp.float32
    )


def transposed_times(left, right):
    return lax.dot_general(
        left, right, (((0,), (0,)), ((), ())), preferred_element_type=jnp.float32
    )


def weight_terms(value_group, normed_all, down_grad, upstream_all):
    values = jnp.dot(normed_all, value_group, preferred_element_type=jnp.float32).astype(
        jnp.bfloat16
    )
    return (transposed_times(normed_all, down_grad), transposed_times(values, upstream_all))


def body(
    w_value,
    w_out,
    norm_gain,
    saved_inputs,
    arriving,
    returning,
    fresh_rows,
    targets,
    fill_slots,
    read_slots,
):
    value_mats = w_value[0]
    out_mats = w_out[0]
    gains = norm_gain[0]
    saved = saved_inputs[0]
    activations = arriving[0]
    cotangents = returning[0]
    tick_count = fresh_rows.shape[0]
    tok_rows = activations.shape[1]
    all_rows = tok_rows * lax.axis_size("dp")
    section_index = lax.axis_index("section")
    last_section = lax.axis_size("section") - 1
    row_offset = lax.axis_index("dp") * tok_rows
    activations, new_rows = (
        lax.all_gather(activations, "dp", axis=1, tiled=True),
        lax.all_gather(fresh_rows, "dp", axis=1, tiled=True),
    )

    def own_rows(block):
        return lax.dynamic_slice_in_dim(block, row_offset, tok_rows, 0)

    def forward(block, group):
        scaled, inv_root, normed = normalize(block, gains[group])
        values = jnp.dot(normed, value_mats[group], preferred_element_type=jnp.float32).astype(
            jnp.bfloat16
        )
        summed = lax.psum(
            jnp.dot(values, out_mats[group], preferred_element_type=jnp.float32).astype(
                jnp.bfloat16
            ),
            "dp",
        ).astype(jnp.float32)
        return (block.astype(jnp.float32) + summed).astype(jnp.bfloat16)

    value_sums = [jnp.zeros(value_mats.shape[1:], jnp.float32) for group in range(2)]
    out_sums = [jnp.zeros(out_mats.shape[1:], jnp.float32) for group in range(2)]
    gain_sums = [jnp.zeros(gains.shape[1:], jnp.float32) for group in range(2)]
    outputs = activations
    gradients = cotangents
    for tick_index in range(tick_count):
        if tick_index > 0:
            received = shifted(outputs, "section", 1)
            lower_group = jnp.where(section_index == 0, new_rows[tick_index], received[0])
            upper_group = jnp.where(section_index == 0, received[0], received[1])
            activations = jnp.stack([lower_group, upper_group])
            returned = shifted(gradients, "section", -1)
            finish = (
                own_rows(outputs[1]).astype(jnp.float32)
                - targets[tick_index - 1].astype(jnp.float32)
            ).astype(jnp.bfloat16)
            cotangents = jnp.stack(
                [
                    jnp.where(section_index == last_section, returned[1], returned[0]),
                    jnp.where(section_index == last_section, finish, returned[1]),
                ]
            )
        for group in range(2):
            saved = saved.at[fill_slots[0, tick_index, group], group].set(
                own_rows(activations[group])
            )
        outputs = jnp.stack([forward(activations[0], 0), forward(activations[1], 1)])
        fresh_grads = []
        for group in range(2):
            source = saved[read_slots[0, tick_index, group], group]
            scaled, inv_root, normed = normalize(source, gains[group])
            normed_all, upstream_all = (
                lax.all_gather(normed, "dp", axis=0, tiled=True),
                lax.all_gather(cotangents[group], "dp", axis=0, tiled=True),
            )
            down_grad = times_transposed(upstream_all, out_mats[group]).astype(jnp.bfloat16)
            pulled = lax.psum_scatter(
                times_transposed(down_grad, value_mats[group]).astype(jnp.bfloat16),
                "dp",
                scatter_dimension=0,
                tiled=True,
            ).astype(jnp.float32)
            weighted = pulled * gains[group]
            inner_mean = jnp.mean(weighted * scaled, axis=-1, keepdims=True)
            fresh_grads.append(
                (
                    cotangents[group].astype(jnp.float32)
                    + inv_root * (weighted - scaled * inner_mean)
                ).astype(jnp.bfloat16)
            )
            gain_sums[group] = gain_sums[group] + jnp.sum(pulled * scaled, axis=0)
            value_term, out_term = weight_terms(
                value_mats[group], normed_all, down_grad, upstream_all
            )
            value_sums[group] = value_sums[group] + value_term
            out_sums[group] = out_sums[group] + out_term
        gradients = jnp.stack(fresh_grads)
    grad_scale = (tick_count * all_rows) ** (-0.5)
    gain_total = lax.psum(jnp.stack(gain_sums).astype(jnp.bfloat16), "dp").astype(jnp.float32)
    final_rows = jnp.stack([own_rows(outputs[0]), own_rows(outputs[1])])
    return (
        final_rows[None],
        gradients[None],
        saved[None],
        (jnp.stack(value_sums) * grad_scale).astype(jnp.bfloat16)[None],
        (jnp.stack(out_sums) * grad_scale).astype(jnp.bfloat16)[None],
        (gain_total * grad_scale)[None],
    )


CHUNK = 512
VMEM_GRANT = 60 * 1024 * 1024
MESH = pl.DeviceIdType.MESH


def chunk_loop(width, step):
    size = CHUNK if width % CHUNK == 0 else width
    lax.fori_loop(0, width // size, lambda i, _: step(pl.ds(pl.multiple_of(i * size, size), size)), None, unroll=UNROLL)


UNROLL = 9


def contract_sum(width, term, shape):
    size = CHUNK if width % CHUNK == 0 else width

    def step(i, total):
        return total + term(pl.ds(pl.multiple_of(i * size, size), size))

    return lax.fori_loop(0, width // size, step, jnp.zeros(shape, jnp.float32), unroll=UNROLL)


def relay_kernel(
    sections,
    wv_hbm,
    wo_hbm,
    gain_ref,
    saved_hbm,
    arriving_hbm,
    returning_hbm,
    fresh_hbm,
    targets_hbm,
    fill_ref,
    read_ref,
    activ_hbm,
    cotan_hbm,
    stash_hbm,
    normed_hbm,
    down_hbm,
    vals_hbm,
    up_hbm,
    gain_hbm,
    stash_ref,
    normed_ref,
    down_ref,
    vals_ref,
    up_ref,
    targets_ref,
    wv,
    wo,
    xin,
    cot,
    staged,
    landed,
    peer_stash,
    psend,
    precv,
    moved,
    lhs,
    scaled_own,
    root_own,
    gain_sum,
    gain_send,
    gain_recv,
    w_sem,
    in_sem,
    out_sem,
    ex_send,
    ex_recv,
    sh_send,
    sh_recv,
    st_send,
    st_recv,
    side_send,
    side_recv,
):
    s = lax.axis_index("section")
    d = lax.axis_index("dp")
    peer = 1 - d
    after = lax.rem(s + 1, sections)
    before = lax.rem(s + sections - 1, sections)
    is_last = s // (sections - 1)
    is_first = before // (sections - 1)
    ticks = fresh_hbm.shape[0]
    half, width = arriving_hbm.shape[1:]
    rows = 2 * half
    features = wv.shape[2]
    slots = saved_hbm.shape[0]

    barrier = pltpu.get_barrier_semaphore()
    for target in ((s, peer), (after, d), (before, d), (after, peer), (before, peer)):
        pl.semaphore_signal(barrier, inc=1, device_id=target, device_id_type=MESH)

    def take(index, source, target):
        copy = pltpu.make_async_copy(source, target, in_sem.at[index])
        copy.start()
        return copy

    own_blocks = {}
    for stream in (0, 3, 1, 2):
        source, buffer = (arriving_hbm, xin) if stream < 2 else (returning_hbm, cot)
        own_blocks[stream] = take(stream, source.at[stream % 2], buffer.at[0, stream % 2, 0])

    weight_copies = {}
    for group in range(2):
        for index, (source, target) in enumerate(((wv_hbm, wv), (wo_hbm, wo))):
            weight_copies[group, index] = pltpu.make_async_copy(
                source.at[group], target.at[group], w_sem.at[group, index]
            )
    for key in ((0, 0), (0, 1), (1, 1), (1, 0)):
        weight_copies[key].start()

    own_fresh = take(4, fresh_hbm.at[pl.ds(1, ticks - 1)], xin.at[pl.ds(1, ticks - 1), 2, 0])
    own_targets = take(5, targets_hbm, targets_ref)
    own_stash = take(6, saved_hbm, stash_ref)
    gain_sum[...] = jnp.zeros_like(gain_sum)
    pl.semaphore_wait(barrier, 5)

    def remote(src, dst, send, recv, target):
        return pltpu.make_async_remote_copy(
            src_ref=src, dst_ref=dst, send_sem=send, recv_sem=recv,
            device_id=target, device_id_type=MESH,
        )

    def initial(stream):
        group = stream % 2
        buffer = xin if stream < 2 else cot
        return remote(
            buffer.at[0, group, 0], buffer.at[0, group, 1],
            sh_send.at[0, stream, 1], sh_recv.at[0, stream, 1], (s, peer),
        )

    def stash_copy(index, group):
        return remote(
            staged.at[index, group], landed.at[index, group],
            st_send.at[index, group], st_recv.at[index, group], (s, peer),
        )

    def fresh_copy(tick):
        return remote(
            xin.at[tick, 2, 0], xin.at[tick, 2, 1],
            side_send.at[tick], side_recv.at[tick], (s, peer),
        )

    gain_copy = remote(gain_send, gain_recv, side_send.at[0], side_recv.at[0], (s, peer))
    for stream in (0, 3, 1, 2):
        own_blocks[stream].wait()
        initial(stream).start()
    own_fresh.wait()
    own_targets.wait()

    def whole(block):
        return block.astype(jnp.float32).reshape(rows, block.shape[2])

    def parted(block):
        return block.reshape(2, half, block.shape[1]).astype(jnp.bfloat16)

    def exchange(tick, stream):
        return remote(
            psend.at[tick, stream, 1], precv.at[tick, stream],
            ex_send.at[tick, stream], ex_recv.at[tick, stream], (s, peer),
        )

    def shift(tick, stream, side):
        group = stream % 2
        if stream < 2:
            place, target, buffer = (group + is_last) % 2, after, xin
        else:
            place, target, buffer = (group + is_first) % 2, before, cot
        return remote(
            moved.at[tick, stream], buffer.at[tick + 1, place, side],
            sh_send.at[tick + 1, stream, side], sh_recv.at[tick + 1, stream - group + place, side],
            (target, peer if side else d),
        )

    def finish_copy(tick):
        return remote(
            cot.at[tick + 1, 1, 0], cot.at[tick + 1, 1, 1],
            sh_send.at[tick + 1, 1, 1], sh_recv.at[tick + 1, 3, 1], (s, peer),
        )

    def arrival(tick, stream, side):
        buffer = xin if stream < 2 else cot
        return remote(
            moved.at[0, stream], buffer.at[tick, stream % 2, side],
            sh_send.at[tick, stream, side], sh_recv.at[tick, stream, side], (s, peer),
        )

    def arrive(tick, stream):
        later = tick > 0
        if stream == 0:
            near, far = later & (s != 0), (tick == 0) | (s != 0)
        elif stream == 3:
            near, far = later & (s != sections - 1), None
        else:
            near, far = later, None

        @pl.when(near)
        def _():
            arrival(tick, stream, 0).wait_recv()

        if far is None:
            arrival(tick, stream, 1).wait_recv()
        else:
            @pl.when(far)
            def _():
                arrival(tick, stream, 1).wait_recv()

            @pl.when(later & (s == 0))
            def _():
                fresh_copy(tick).wait_recv()

    def input_place(tick, group):
        return 2 * is_first * jnp.minimum(tick, 1) if group == 0 else 1

    def norm_parts(values, group):
        inv_root = lax.rsqrt(jnp.mean(values * values, axis=-1, keepdims=True) + epsilon)
        scaled = values * inv_root
        return scaled, inv_root, (scaled * gain_ref[pl.ds(group, 1), :]).astype(jnp.bfloat16)

    def weights_ready(tick, key):
        @pl.when(tick == 0)
        def _():
            weight_copies[key].wait()

    def stash_sends(tick, group):
        @pl.when(tick == ticks - 1)
        def _():
            for index in range(slots - 1):
                stash_copy(index, group).start()

    def exchanged(tick, stream):
        return (s != 0) | (tick == ticks - 1) if stream == 2 else tick >= 0

    def forward_start(tick, group):
        arrive(tick, group)
        lhs[...] = norm_parts(whole(xin[tick, input_place(tick, group)]), group)[2]
        if group == 0:
            weights_ready(tick, (0, 0))
        values = contract_sum(
            width,
            lambda at: jnp.dot(lhs[:, at], wv[group, at, :], preferred_element_type=jnp.float32),
            (rows, features),
        ).astype(jnp.bfloat16)
        if group == 0:
            weights_ready(tick, (0, 1))

        def step(at):
            psend[tick, group, :, :, at] = parted(
                jnp.dot(values, wo[group, :, at], preferred_element_type=jnp.float32)
            )

        chunk_loop(width, step)
        exchange(tick, group).start()

    def peer_sum(tick, stream):
        exchange(tick, stream).wait_recv()
        return psend[tick, stream, 0].astype(jnp.float32) + precv[tick, stream].astype(jnp.float32)

    def forward_finish(tick, group):
        own = xin[tick, input_place(tick, group), 0].astype(jnp.float32)
        outputs = (own + peer_sum(tick, group)).astype(jnp.bfloat16)
        moved[tick, group] = outputs
        going = tick < ticks - 1

        @pl.when(going if group == 0 else going & (s != sections - 1))
        def _():
            shift(tick, group, 1).start()
            shift(tick, group, 0).start()

        if group == 1:
            @pl.when(going & (s == sections - 1))
            def _():
                cot[tick + 1, 1, 0] = (
                    outputs.astype(jnp.float32) - targets_ref[tick].astype(jnp.float32)
                ).astype(jnp.bfloat16)
                finish_copy(tick).start()

    def backward_start(tick, group):
        arrive(tick, 2 + group)
        up_ref[group, tick] = whole(cot[tick, group]).astype(jnp.bfloat16)
        if group == 1:
            weights_ready(tick, (1, 1))
        down = contract_sum(
            width,
            lambda at: times_transposed(up_ref[group, tick, :, at], wo[group, :, at]),
            (rows, features),
        ).astype(jnp.bfloat16)
        down_ref[group, tick] = down
        if group == 1:
            weights_ready(tick, (1, 0))

        def step(at):
            psend[tick, 2 + group, :, :, at] = parted(times_transposed(down, wv[group, at, :]))

        chunk_loop(width, step)

        @pl.when(exchanged(tick, 2 + group))
        def _():
            exchange(tick, 2 + group).start()

        if group == 0:
            @pl.when((tick < ticks - 1) & (s == 0))
            def _():
                fresh_copy(tick + 1).start()

    def own_source(tick, group):
        @pl.when(tick == 0)
        def _():
            if group == 1:
                own_stash.wait()
            for index in range(slots - 1):
                staged[index, group] = jnp.where(
                    fill_ref[group, 0] <= index, stash_ref[index + 1, group], stash_ref[index, group]
                )

        block = xin[tick, input_place(tick, group), 0]
        for slot in range(slots):
            stash_ref[slot, group] = jnp.where(fill_ref[group, tick] == slot, block, stash_ref[slot, group])
        source = stash_ref[read_ref[group, tick], group].astype(jnp.float32)
        scaled, inv_root, normed = norm_parts(source, group)
        normed_ref[group, tick, 0] = normed
        scaled_own[group] = scaled
        root_own[group] = jnp.broadcast_to(inv_root, root_own.shape[1:])
        gain_sum[group] += psend[tick, 2 + group, 0].astype(jnp.float32) * scaled

    def peer_stash_start(group):
        filled = fill_ref[group, 0]
        for index in range(slots - 1):
            stash_copy(index, group).wait_recv()
        for slot in range(slots):
            low, high = max(slot - 1, 0), min(slot, slots - 2)
            peer_stash[slot, group] = jnp.where(filled < slot, landed[low, group], landed[high, group])

    def peer_source(tick, group):
        block = xin[tick, input_place(tick, group), 1]
        for slot in range(slots):
            peer_stash[slot, group] = jnp.where(
                fill_ref[group, tick] == slot, block, peer_stash[slot, group]
            )
        source = peer_stash[read_ref[group, tick], group].astype(jnp.float32)
        scaled, _, normed = norm_parts(source, group)
        normed_ref[group, tick, 1] = normed
        gain_sum[group] += psend[tick, 2 + group, 1].astype(jnp.float32) * scaled

    def gradient(tick, group):
        scaled = scaled_own[group]
        pulled = peer_sum(tick, 2 + group)
        weighted = pulled * gain_ref[pl.ds(group, 1), :]
        inner_mean = jnp.mean(weighted * scaled, axis=-1, keepdims=True)
        moved[tick, 2 + group] = (
            cot[tick, group, 0].astype(jnp.float32)
            + root_own[group][:, :1] * (weighted - scaled * inner_mean)
        ).astype(jnp.bfloat16)

    def backward_finish(tick, group):
        @pl.when(exchanged(tick, 2 + group))
        def _():
            gradient(tick, group)

            @pl.when(tick < ticks - 1)
            def _():
                shift(tick, 2 + group, 1).start()
                shift(tick, 2 + group, 0).start()

    def tick_step(tick, _):
        forward_start(tick, 0)
        backward_start(tick, 1)

        @pl.when(tick > 0)
        def _():
            backward_finish(tick - 1, 0)

        stash_sends(tick, 1)
        forward_finish(tick, 0)
        forward_start(tick, 1)
        stash_sends(tick, 0)
        own_source(tick, 1)
        backward_finish(tick, 1)
        backward_start(tick, 0)
        own_source(tick, 0)
        forward_finish(tick, 1)
        return None

    lax.fori_loop(0, ticks, tick_step, None)

    def give(index, source, target):
        copy = pltpu.make_async_copy(source, target, out_sem.at[index])
        copy.start()
        return copy

    given = [
        give(0, stash_ref, stash_hbm),
        give(1, up_ref, up_hbm),
        give(2, down_ref, down_hbm),
        give(3, moved.at[ticks - 1, pl.ds(0, 2)], activ_hbm),
    ]
    for group in (1, 0):
        peer_stash_start(group)

        def source_step(tick, _):
            peer_source(tick, group)
            return None

        lax.fori_loop(0, ticks, source_step, None)
        given.append(give(4 + group, normed_ref.at[group], normed_hbm.at[group]))
        gain_send[pl.ds(group, 1), :] = jnp.sum(gain_sum[group], axis=0, keepdims=True)
    gain_copy.start()
    for group in range(2):
        def chunk_values(at):
            block = normed_ref[group, :, :, :, at].astype(jnp.float32)
            left = block.reshape(ticks * rows, block.shape[3]).astype(jnp.bfloat16)
            return jnp.dot(left, wv[group, at, :], preferred_element_type=jnp.float32)

        vals_ref[group] = contract_sum(width, chunk_values, (ticks * rows, features)).astype(jnp.bfloat16)
    given.append(give(6, vals_ref, vals_hbm))
    backward_finish(ticks - 1, 0)
    given.append(give(7, moved.at[ticks - 1, pl.ds(2, 2)], cotan_hbm))
    gain_copy.wait_recv()
    gain_sum[0, pl.ds(0, 2), :] = (gain_send[...] + gain_recv[...]) * (ticks * rows) ** (-0.5)
    given.append(give(8, gain_sum.at[0, pl.ds(0, 2)], gain_hbm))
    for copy in given:
        copy.wait()

    gain_copy.wait_send()
    for stream in range(4):
        initial(stream).wait_send()
    for group in range(2):
        for index in range(slots - 1):
            stash_copy(index, group).wait_send()

    @pl.when(s == 0)
    def _():
        for tick in range(1, ticks):
            fresh_copy(tick).wait_send()

    for tick in range(ticks):
        for stream in range(4):
            @pl.when(exchanged(tick, stream))
            def _():
                exchange(tick, stream).wait_send()
    for tick in range(ticks - 1):
        for side in range(2):
            shift(tick, 0, side).wait_send()
            shift(tick, 3, side).wait_send()

        @pl.when(s != sections - 1)
        def _():
            for side in range(2):
                shift(tick, 1, side).wait_send()

        @pl.when(s == sections - 1)
        def _():
            finish_copy(tick).wait_send()

        @pl.when(s != 0)
        def _():
            for side in range(2):
                shift(tick, 2, side).wait_send()


def grads_kernel(
    grad_scale, activ_ref, cotan_ref, stash_ref, gain_ref, normed_ref, down_ref, vals_ref, up_ref,
    activ_hbm, cotan_hbm, stash_hbm, value_hbm, out_hbm, gain_hbm,
    value_grad, out_grad, small_sem, grad_sem,
):
    small = [
        pltpu.make_async_copy(source, target, small_sem.at[index])
        for index, (source, target) in enumerate(
            ((activ_ref, activ_hbm), (cotan_ref, cotan_hbm), (stash_ref, stash_hbm), (gain_ref, gain_hbm))
        )
    ]
    for copy in small:
        copy.start()
    width = normed_ref.shape[2]
    size = CHUNK if width % CHUNK == 0 else width

    def step(index, _):
        at = pl.ds(pl.multiple_of(index * size, size), size)
        for group in range(2):
            value_grad[group, at, :] = (
                transposed_times(normed_ref[group, :, at], down_ref[group]) * grad_scale
            ).astype(jnp.bfloat16)
            pltpu.make_async_copy(
                value_grad.at[group, at, :], value_hbm.at[group, at, :], grad_sem.at[0]
            ).start()
            out_grad[group, :, at] = (
                transposed_times(vals_ref[group], up_ref[group, :, at]) * grad_scale
            ).astype(jnp.bfloat16)
            pltpu.make_async_copy(
                out_grad.at[group, :, at], out_hbm.at[group, :, at], grad_sem.at[1]
            ).start()
        return None

    lax.fori_loop(0, width // size, step, None)
    pltpu.make_async_copy(value_grad, value_hbm, grad_sem.at[0]).wait()
    pltpu.make_async_copy(out_grad, out_hbm, grad_sem.at[1]).wait()
    for copy in small:
        copy.wait()


def relay_body(
    sections,
    w_value,
    w_out,
    norm_gain,
    saved_inputs,
    arriving,
    returning,
    fresh_rows,
    targets,
    fill_slots,
    read_slots,
):
    value_mats, out_mats, gains = w_value[0], w_out[0], norm_gain[0]
    saved, activations, cotangents = saved_inputs[0], arriving[0], returning[0]
    ticks, half, width = fresh_rows.shape
    features = value_mats.shape[2]
    slots = saved.shape[0]
    if slots < 2:
        return body(
            w_value, w_out, norm_gain, saved_inputs, arriving,
            returning, fresh_rows, targets, fill_slots, read_slots,
        )
    rows = 2 * half
    vmem = pl.BlockSpec(memory_space=pltpu.VMEM)
    smem = pl.BlockSpec(memory_space=pltpu.SMEM)
    hbm = pl.BlockSpec(memory_space=pl.ANY)
    shape = jax.ShapeDtypeStruct
    narrow = jnp.bfloat16
    final_rows, gradients, stash_rows, normed, down, values, upstream, gain_sums = pl.pallas_call(
        functools.partial(relay_kernel, sections),
        out_shape=(
            shape(activations.shape, narrow),
            shape(cotangents.shape, narrow),
            shape(saved.shape, narrow),
            shape((2, ticks, 2, half, width), narrow),
            shape((2, ticks, rows, features), narrow),
            shape((2, ticks * rows, features), narrow),
            shape((2, ticks, rows, width), narrow),
            shape(gains.shape, jnp.float32),
        ),
        in_specs=[hbm, hbm, vmem] + [hbm] * 5 + [smem] * 2,
        out_specs=(hbm,) * 8,
        scratch_shapes=[
            pltpu.VMEM(saved.shape, narrow),
            pltpu.VMEM((2, ticks, 2, half, width), narrow),
            pltpu.VMEM((2, ticks, rows, features), narrow),
            pltpu.VMEM((2, ticks * rows, features), narrow),
            pltpu.VMEM((2, ticks, rows, width), narrow),
            pltpu.VMEM((ticks, half, width), narrow),
            pltpu.VMEM(value_mats.shape, narrow),
            pltpu.VMEM(out_mats.shape, narrow),
            pltpu.VMEM((ticks, 3, 2, half, width), narrow),
            pltpu.VMEM((ticks, 2, 2, half, width), narrow),
            pltpu.VMEM((slots - 1, 2, half, width), narrow),
            pltpu.VMEM((slots - 1, 2, half, width), narrow),
            pltpu.VMEM((slots, 2, half, width), narrow),
            pltpu.VMEM((ticks, 4, 2, half, width), narrow),
            pltpu.VMEM((ticks, 4, half, width), narrow),
            pltpu.VMEM((ticks, 4, half, width), narrow),
            pltpu.VMEM((rows, width), narrow),
            pltpu.VMEM((2, half, width), jnp.float32),
            pltpu.VMEM((2, half, 128), jnp.float32),
            pltpu.VMEM((2, half, width), jnp.float32),
            pltpu.VMEM((2, width), jnp.float32),
            pltpu.VMEM((2, width), jnp.float32),
            pltpu.SemaphoreType.DMA((2, 2)),
            pltpu.SemaphoreType.DMA((7,)),
            pltpu.SemaphoreType.DMA((9,)),
            pltpu.SemaphoreType.DMA((ticks, 4)),
            pltpu.SemaphoreType.DMA((ticks, 4)),
            pltpu.SemaphoreType.DMA((ticks, 4, 2)),
            pltpu.SemaphoreType.DMA((ticks, 4, 2)),
            pltpu.SemaphoreType.DMA((slots - 1, 2)),
            pltpu.SemaphoreType.DMA((slots - 1, 2)),
            pltpu.SemaphoreType.DMA((ticks,)),
            pltpu.SemaphoreType.DMA((ticks,)),
        ],
        compiler_params=pltpu.CompilerParams(
            collective_id=0, has_side_effects=True, vmem_limit_bytes=VMEM_GRANT
        ),
    )(
        value_mats, out_mats, gains, saved, activations, cotangents,
        fresh_rows, targets, fill_slots[0].T, read_slots[0].T,
    )
    flat = lambda block: block.reshape(2, ticks * rows, block.shape[-1])
    grads = pl.pallas_call(
        functools.partial(grads_kernel, (ticks * rows) ** (-0.5)),
        out_shape=(
            shape(activations.shape, narrow),
            shape(cotangents.shape, narrow),
            shape(saved.shape, narrow),
            shape(value_mats.shape, narrow),
            shape(out_mats.shape, narrow),
            shape(gains.shape, jnp.float32),
        ),
        in_specs=[vmem] * 8,
        out_specs=(hbm,) * 6,
        scratch_shapes=[
            pltpu.VMEM(value_mats.shape, narrow),
            pltpu.VMEM(out_mats.shape, narrow),
            pltpu.SemaphoreType.DMA((4,)),
            pltpu.SemaphoreType.DMA((2,)),
        ],
        compiler_params=pltpu.CompilerParams(vmem_limit_bytes=VMEM_GRANT),
    )(final_rows, gradients, stash_rows, gain_sums, flat(normed), flat(down), flat(values), flat(upstream))
    return tuple(block[None] for block in grads)


def solution(mesh):
    in_specs = (
        P("section", None, None, "dp"),
        P("section", None, "dp", None),
        P("section", None, None),
        P("section", None, None, "dp", None),
        P("section", None, "dp", None),
        P("section", None, "dp", None),
        P(None, "dp", None),
        P(None, "dp", None),
        P("section", None, None),
        P("section", None, None),
    )
    out_specs = (
        P("section", None, "dp", None),
        P("section", None, "dp", None),
        P("section", None, None, "dp", None),
        P("section", None, None, "dp"),
        P("section", None, "dp", None),
        P("section", None, None),
    )
    paired = mesh.shape["dp"] == 2 and mesh.shape["section"] > 2
    program = functools.partial(relay_body, mesh.shape["section"]) if paired else body
    return jax.shard_map(program, mesh=mesh, in_specs=in_specs, out_specs=out_specs, check_vma=False)
```

```python
import functools

import jax
import jax.numpy as jnp
from jax import lax
from jax.experimental import pallas as pl
from jax.experimental.pallas import tpu as pltpu
from jax.sharding import PartitionSpec as P

epsilon = 1e-06


def shifted(shard, axis, by):
    devices = lax.axis_size(axis)
    return lax.ppermute(shard, axis, [(i, (i + by) % devices) for i in range(devices)])


def normalize(block_rows, gain_row):
    values = block_rows.astype(jnp.float32)
    inv_root = lax.rsqrt(jnp.mean(values * values, axis=-1, keepdims=True) + epsilon)
    scaled = values * inv_root
    return (scaled, inv_root, (scaled * gain_row).astype(jnp.bfloat16))


def times_transposed(left, right):
    return lax.dot_general(
        left, right, (((1,), (1,)), ((), ())), preferred_element_type=jnp.float32
    )


def transposed_times(left, right):
    return lax.dot_general(
        left, right, (((0,), (0,)), ((), ())), preferred_element_type=jnp.float32
    )


def weight_terms(value_group, normed_all, down_grad, upstream_all):
    values = jnp.dot(normed_all, value_group, preferred_element_type=jnp.float32).astype(
        jnp.bfloat16
    )
    return (transposed_times(normed_all, down_grad), transposed_times(values, upstream_all))


def body(
    w_value,
    w_out,
    norm_gain,
    saved_inputs,
    arriving,
    returning,
    fresh_rows,
    targets,
    fill_slots,
    read_slots,
):
    value_mats = w_value[0]
    out_mats = w_out[0]
    gains = norm_gain[0]
    saved = saved_inputs[0]
    activations = arriving[0]
    cotangents = returning[0]
    tick_count = fresh_rows.shape[0]
    tok_rows = activations.shape[1]
    all_rows = tok_rows * lax.axis_size("dp")
    section_index = lax.axis_index("section")
    last_section = lax.axis_size("section") - 1
    row_offset = lax.axis_index("dp") * tok_rows
    activations, new_rows = (
        lax.all_gather(activations, "dp", axis=1, tiled=True),
        lax.all_gather(fresh_rows, "dp", axis=1, tiled=True),
    )

    def own_rows(block):
        return lax.dynamic_slice_in_dim(block, row_offset, tok_rows, 0)

    def forward(block, group):
        scaled, inv_root, normed = normalize(block, gains[group])
        values = jnp.dot(normed, value_mats[group], preferred_element_type=jnp.float32).astype(
            jnp.bfloat16
        )
        summed = lax.psum(
            jnp.dot(values, out_mats[group], preferred_element_type=jnp.float32).astype(
                jnp.bfloat16
            ),
            "dp",
        ).astype(jnp.float32)
        return (block.astype(jnp.float32) + summed).astype(jnp.bfloat16)

    value_sums = [jnp.zeros(value_mats.shape[1:], jnp.float32) for group in range(2)]
    out_sums = [jnp.zeros(out_mats.shape[1:], jnp.float32) for group in range(2)]
    gain_sums = [jnp.zeros(gains.shape[1:], jnp.float32) for group in range(2)]
    outputs = activations
    gradients = cotangents
    for tick_index in range(tick_count):
        if tick_index > 0:
            received = shifted(outputs, "section", 1)
            lower_group = jnp.where(section_index == 0, new_rows[tick_index], received[0])
            upper_group = jnp.where(section_index == 0, received[0], received[1])
            activations = jnp.stack([lower_group, upper_group])
            returned = shifted(gradients, "section", -1)
            finish = (
                own_rows(outputs[1]).astype(jnp.float32)
                - targets[tick_index - 1].astype(jnp.float32)
            ).astype(jnp.bfloat16)
            cotangents = jnp.stack(
                [
                    jnp.where(section_index == last_section, returned[1], returned[0]),
                    jnp.where(section_index == last_section, finish, returned[1]),
                ]
            )
        for group in range(2):
            saved = saved.at[fill_slots[0, tick_index, group], group].set(
                own_rows(activations[group])
            )
        outputs = jnp.stack([forward(activations[0], 0), forward(activations[1], 1)])
        fresh_grads = []
        for group in range(2):
            source = saved[read_slots[0, tick_index, group], group]
            scaled, inv_root, normed = normalize(source, gains[group])
            normed_all, upstream_all = (
                lax.all_gather(normed, "dp", axis=0, tiled=True),
                lax.all_gather(cotangents[group], "dp", axis=0, tiled=True),
            )
            down_grad = times_transposed(upstream_all, out_mats[group]).astype(jnp.bfloat16)
            pulled = lax.psum_scatter(
                times_transposed(down_grad, value_mats[group]).astype(jnp.bfloat16),
                "dp",
                scatter_dimension=0,
                tiled=True,
            ).astype(jnp.float32)
            weighted = pulled * gains[group]
            inner_mean = jnp.mean(weighted * scaled, axis=-1, keepdims=True)
            fresh_grads.append(
                (
                    cotangents[group].astype(jnp.float32)
                    + inv_root * (weighted - scaled * inner_mean)
                ).astype(jnp.bfloat16)
            )
            gain_sums[group] = gain_sums[group] + jnp.sum(pulled * scaled, axis=0)
            value_term, out_term = weight_terms(
                value_mats[group], normed_all, down_grad, upstream_all
            )
            value_sums[group] = value_sums[group] + value_term
            out_sums[group] = out_sums[group] + out_term
        gradients = jnp.stack(fresh_grads)
    grad_scale = (tick_count * all_rows) ** (-0.5)
    gain_total = lax.psum(jnp.stack(gain_sums).astype(jnp.bfloat16), "dp").astype(jnp.float32)
    final_rows = jnp.stack([own_rows(outputs[0]), own_rows(outputs[1])])
    return (
        final_rows[None],
        gradients[None],
        saved[None],
        (jnp.stack(value_sums) * grad_scale).astype(jnp.bfloat16)[None],
        (jnp.stack(out_sums) * grad_scale).astype(jnp.bfloat16)[None],
        (gain_total * grad_scale)[None],
    )


CHUNK = 512
VMEM_GRANT = 60 * 1024 * 1024
MESH = pl.DeviceIdType.MESH


def chunk_loop(width, step):
    size = CHUNK if width % CHUNK == 0 else width
    lax.fori_loop(0, width // size, lambda i, _: step(pl.ds(pl.multiple_of(i * size, size), size)), None, unroll=UNROLL)


UNROLL = 9


def contract_sum(width, term, shape):
    size = CHUNK if width % CHUNK == 0 else width

    def step(i, total):
        return total + term(pl.ds(pl.multiple_of(i * size, size), size))

    return lax.fori_loop(0, width // size, step, jnp.zeros(shape, jnp.float32), unroll=UNROLL)


def input_gradient(pulled, cotangent, scaled, root, gain_row):
    weighted = pulled * gain_row
    inner_mean = jnp.mean(weighted * scaled, axis=-1, keepdims=True)
    return (
        cotangent.astype(jnp.float32) + root[:, :1] * (weighted - scaled * inner_mean)
    ).astype(jnp.bfloat16)


def relay_kernel(
    sections,
    wv_hbm,
    wo_hbm,
    gain_ref,
    saved_hbm,
    arriving_hbm,
    returning_hbm,
    fresh_hbm,
    targets_hbm,
    fill_ref,
    read_ref,
    part_own_hbm,
    part_peer_hbm,
    input_hbm,
    cot_hbm,
    scaled_hbm,
    root_hbm,
    stash_hbm,
    normed_hbm,
    down_hbm,
    vals_hbm,
    up_hbm,
    gain_hbm,
    stash_ref,
    normed_ref,
    down_ref,
    vals_ref,
    up_ref,
    targets_ref,
    wv,
    wo,
    xin,
    cot,
    staged,
    landed,
    peer_stash,
    psend,
    precv,
    moved,
    lhs,
    scaled_own,
    root_own,
    gain_sum,
    gain_send,
    gain_recv,
    w_sem,
    in_sem,
    out_sem,
    ex_send,
    ex_recv,
    sh_send,
    sh_recv,
    st_send,
    st_recv,
    side_send,
    side_recv,
):
    s = lax.axis_index("section")
    d = lax.axis_index("dp")
    peer = 1 - d
    after = lax.rem(s + 1, sections)
    before = lax.rem(s + sections - 1, sections)
    is_last = s // (sections - 1)
    is_first = before // (sections - 1)
    ticks = fresh_hbm.shape[0]
    half, width = arriving_hbm.shape[1:]
    rows = 2 * half
    features = wv.shape[2]
    slots = saved_hbm.shape[0]

    barrier = pltpu.get_barrier_semaphore()
    for target in ((s, peer), (after, d), (before, d), (after, peer), (before, peer)):
        pl.semaphore_signal(barrier, inc=1, device_id=target, device_id_type=MESH)

    def take(index, source, target):
        copy = pltpu.make_async_copy(source, target, in_sem.at[index])
        copy.start()
        return copy

    own_blocks = {}
    for stream in (0, 3, 1, 2):
        source, buffer = (arriving_hbm, xin) if stream < 2 else (returning_hbm, cot)
        own_blocks[stream] = take(stream, source.at[stream % 2], buffer.at[0, stream % 2, 0])

    weight_copies = {}
    for group in range(2):
        for index, (source, target) in enumerate(((wv_hbm, wv), (wo_hbm, wo))):
            weight_copies[group, index] = pltpu.make_async_copy(
                source.at[group], target.at[group], w_sem.at[group, index]
            )
    for key in ((0, 0), (0, 1), (1, 1), (1, 0)):
        weight_copies[key].start()

    own_fresh = take(4, fresh_hbm.at[pl.ds(1, ticks - 1)], xin.at[pl.ds(1, ticks - 1), 2, 0])
    own_targets = take(5, targets_hbm, targets_ref)
    own_stash = take(6, saved_hbm, stash_ref)
    gain_sum[...] = jnp.zeros_like(gain_sum)
    pl.semaphore_wait(barrier, 5)

    def remote(src, dst, send, recv, target):
        return pltpu.make_async_remote_copy(
            src_ref=src, dst_ref=dst, send_sem=send, recv_sem=recv,
            device_id=target, device_id_type=MESH,
        )

    def initial(stream):
        group = stream % 2
        buffer = xin if stream < 2 else cot
        return remote(
            buffer.at[0, group, 0], buffer.at[0, group, 1],
            sh_send.at[0, stream, 1], sh_recv.at[0, stream, 1], (s, peer),
        )

    def stash_copy(index, group):
        return remote(
            staged.at[index, group], landed.at[index, group],
            st_send.at[index, group], st_recv.at[index, group], (s, peer),
        )

    def fresh_copy(tick):
        return remote(
            xin.at[tick, 2, 0], xin.at[tick, 2, 1],
            side_send.at[tick], side_recv.at[tick], (s, peer),
        )

    gain_copy = remote(gain_send, gain_recv, side_send.at[0], side_recv.at[0], (s, peer))
    for stream in (0, 3, 1, 2):
        own_blocks[stream].wait()
        initial(stream).start()
    own_fresh.wait()
    own_targets.wait()

    def whole(block):
        return block.astype(jnp.float32).reshape(rows, block.shape[2])

    def parted(block):
        return block.reshape(2, half, block.shape[1]).astype(jnp.bfloat16)

    def exchange(tick, stream):
        return remote(
            psend.at[tick, stream, 1], precv.at[tick, stream],
            ex_send.at[tick, stream], ex_recv.at[tick, stream], (s, peer),
        )

    def shift(tick, stream, side):
        group = stream % 2
        if stream < 2:
            place, target, buffer = (group + is_last) % 2, after, xin
        else:
            place, target, buffer = (group + is_first) % 2, before, cot
        return remote(
            moved.at[tick, stream], buffer.at[tick + 1, place, side],
            sh_send.at[tick + 1, stream, side], sh_recv.at[tick + 1, stream - group + place, side],
            (target, peer if side else d),
        )

    def finish_copy(tick):
        return remote(
            cot.at[tick + 1, 1, 0], cot.at[tick + 1, 1, 1],
            sh_send.at[tick + 1, 1, 1], sh_recv.at[tick + 1, 3, 1], (s, peer),
        )

    def arrival(tick, stream, side):
        buffer = xin if stream < 2 else cot
        return remote(
            moved.at[0, stream], buffer.at[tick, stream % 2, side],
            sh_send.at[tick, stream, side], sh_recv.at[tick, stream, side], (s, peer),
        )

    def arrive(tick, stream):
        later = tick > 0
        if stream == 0:
            near, far = later & (s != 0), (tick == 0) | (s != 0)
        elif stream == 3:
            near, far = later & (s != sections - 1), None
        else:
            near, far = later, None

        @pl.when(near)
        def _():
            arrival(tick, stream, 0).wait_recv()

        if far is None:
            arrival(tick, stream, 1).wait_recv()
        else:
            @pl.when(far)
            def _():
                arrival(tick, stream, 1).wait_recv()

            @pl.when(later & (s == 0))
            def _():
                fresh_copy(tick).wait_recv()

    def input_place(tick, group):
        return 2 * is_first * jnp.minimum(tick, 1) if group == 0 else 1

    def norm_parts(values, group):
        inv_root = lax.rsqrt(jnp.mean(values * values, axis=-1, keepdims=True) + epsilon)
        scaled = values * inv_root
        return scaled, inv_root, (scaled * gain_ref[pl.ds(group, 1), :]).astype(jnp.bfloat16)

    def weights_ready(tick, key):
        @pl.when(tick == 0)
        def _():
            weight_copies[key].wait()

    def stash_sends(tick, group):
        @pl.when(tick == ticks - 1)
        def _():
            for index in range(slots - 1):
                stash_copy(index, group).start()

    def exchanged(tick, stream):
        going = tick < ticks - 1
        return going & (s != 0) if stream == 2 else going

    def forward_start(tick, group):
        arrive(tick, group)
        lhs[...] = norm_parts(whole(xin[tick, input_place(tick, group)]), group)[2]
        if group == 0:
            weights_ready(tick, (0, 0))
        values = contract_sum(
            width,
            lambda at: jnp.dot(lhs[:, at], wv[group, at, :], preferred_element_type=jnp.float32),
            (rows, features),
        ).astype(jnp.bfloat16)
        if group == 0:
            weights_ready(tick, (0, 1))

        def step(at):
            psend[tick, group, :, :, at] = parted(
                jnp.dot(values, wo[group, :, at], preferred_element_type=jnp.float32)
            )

        chunk_loop(width, step)

        @pl.when(exchanged(tick, group))
        def _():
            exchange(tick, group).start()

    def peer_sum(tick, stream):
        exchange(tick, stream).wait_recv()
        return psend[tick, stream, 0].astype(jnp.float32) + precv[tick, stream].astype(jnp.float32)

    def forward_finish(tick, group):
        @pl.when(exchanged(tick, group))
        def _():
            own = xin[tick, input_place(tick, group), 0].astype(jnp.float32)
            outputs = (own + peer_sum(tick, group)).astype(jnp.bfloat16)
            moved[tick, group] = outputs

            def send_on():
                shift(tick, group, 1).start()
                shift(tick, group, 0).start()

            if group == 0:
                send_on()
            else:
                pl.when(s != sections - 1)(send_on)

                @pl.when(s == sections - 1)
                def _():
                    cot[tick + 1, 1, 0] = (
                        outputs.astype(jnp.float32) - targets_ref[tick].astype(jnp.float32)
                    ).astype(jnp.bfloat16)
                    finish_copy(tick).start()

    def backward_start(tick, group):
        arrive(tick, 2 + group)
        up_ref[group, tick] = whole(cot[tick, group]).astype(jnp.bfloat16)
        if group == 1:
            weights_ready(tick, (1, 1))
        down = contract_sum(
            width,
            lambda at: times_transposed(up_ref[group, tick, :, at], wo[group, :, at]),
            (rows, features),
        ).astype(jnp.bfloat16)
        down_ref[group, tick] = down
        if group == 1:
            weights_ready(tick, (1, 0))

        def step(at):
            psend[tick, 2 + group, :, :, at] = parted(times_transposed(down, wv[group, at, :]))

        chunk_loop(width, step)

        @pl.when(exchanged(tick, 2 + group))
        def _():
            exchange(tick, 2 + group).start()

        if group == 0:
            @pl.when((tick < ticks - 1) & (s == 0))
            def _():
                fresh_copy(tick + 1).start()

    def own_source(tick, group):
        @pl.when(tick == 0)
        def _():
            if group == 1:
                own_stash.wait()
            for index in range(slots - 1):
                staged[index, group] = jnp.where(
                    fill_ref[group, 0] <= index, stash_ref[index + 1, group], stash_ref[index, group]
                )

        block = xin[tick, input_place(tick, group), 0]
        for slot in range(slots):
            stash_ref[slot, group] = jnp.where(fill_ref[group, tick] == slot, block, stash_ref[slot, group])
        source = stash_ref[read_ref[group, tick], group].astype(jnp.float32)
        scaled, inv_root, normed = norm_parts(source, group)
        normed_ref[group, tick, 0] = normed
        scaled_own[group] = scaled
        root_own[group] = jnp.broadcast_to(inv_root, root_own.shape[1:])
        gain_sum[group] += psend[tick, 2 + group, 0].astype(jnp.float32) * scaled

    def peer_stash_start(group):
        filled = fill_ref[group, 0]
        for index in range(slots - 1):
            stash_copy(index, group).wait_recv()
        for slot in range(slots):
            low, high = max(slot - 1, 0), min(slot, slots - 2)
            peer_stash[slot, group] = jnp.where(filled < slot, landed[low, group], landed[high, group])

    def peer_source(tick, group):
        block = xin[tick, input_place(tick, group), 1]
        for slot in range(slots):
            peer_stash[slot, group] = jnp.where(
                fill_ref[group, tick] == slot, block, peer_stash[slot, group]
            )
        source = peer_stash[read_ref[group, tick], group].astype(jnp.float32)
        scaled, _, normed = norm_parts(source, group)
        normed_ref[group, tick, 1] = normed
        gain_sum[group] += psend[tick, 2 + group, 1].astype(jnp.float32) * scaled

    def backward_finish(tick, group):
        @pl.when(exchanged(tick, 2 + group))
        def _():
            pulled = peer_sum(tick, 2 + group)
            moved[tick, 2 + group] = input_gradient(
                pulled, cot[tick, group, 0], scaled_own[group], root_own[group], gain_ref[pl.ds(group, 1), :]
            )
            shift(tick, 2 + group, 1).start()
            shift(tick, 2 + group, 0).start()

    def tick_step(tick, _):
        forward_start(tick, 0)
        backward_start(tick, 1)

        @pl.when(tick > 0)
        def _():
            backward_finish(tick - 1, 0)

        stash_sends(tick, 1)
        forward_finish(tick, 0)
        forward_start(tick, 1)
        stash_sends(tick, 0)
        own_source(tick, 1)
        backward_finish(tick, 1)
        backward_start(tick, 0)
        own_source(tick, 0)
        forward_finish(tick, 1)
        return None

    lax.fori_loop(0, ticks, tick_step, None)

    def give(index, source, target):
        copy = pltpu.make_async_copy(source, target, out_sem.at[index])
        copy.start()
        return copy

    last = ticks - 1
    given = [
        give(0, psend.at[last, :, 0], part_own_hbm),
        give(1, psend.at[last, :, 1], part_peer_hbm),
        give(2, xin.at[last, input_place(last, 0), 0], input_hbm.at[0]),
        give(3, xin.at[last, 1, 0], input_hbm.at[1]),
        give(4, cot.at[last, :, 0], cot_hbm),
        give(5, scaled_own, scaled_hbm),
        give(6, root_own, root_hbm),
        give(7, stash_ref, stash_hbm),
        give(8, up_ref, up_hbm),
        give(9, down_ref, down_hbm),
    ]
    for group in (1, 0):
        peer_stash_start(group)

        def source_step(tick, _):
            peer_source(tick, group)
            return None

        lax.fori_loop(0, ticks, source_step, None)
        given.append(give(10 + group, normed_ref.at[group], normed_hbm.at[group]))
        gain_send[pl.ds(group, 1), :] = jnp.sum(gain_sum[group], axis=0, keepdims=True)
    gain_copy.start()
    for group in range(2):
        def chunk_values(at):
            block = normed_ref[group, :, :, :, at].astype(jnp.float32)
            left = block.reshape(ticks * rows, block.shape[3]).astype(jnp.bfloat16)
            return jnp.dot(left, wv[group, at, :], preferred_element_type=jnp.float32)

        vals_ref[group] = contract_sum(width, chunk_values, (ticks * rows, features)).astype(jnp.bfloat16)
    given.append(give(12, vals_ref, vals_hbm))
    gain_copy.wait_recv()
    gain_sum[0, pl.ds(0, 2), :] = (gain_send[...] + gain_recv[...]) * (ticks * rows) ** (-0.5)
    given.append(give(13, gain_sum.at[0, pl.ds(0, 2)], gain_hbm))
    for copy in given:
        copy.wait()

    gain_copy.wait_send()
    for stream in range(4):
        initial(stream).wait_send()
    for group in range(2):
        for index in range(slots - 1):
            stash_copy(index, group).wait_send()

    @pl.when(s == 0)
    def _():
        for tick in range(1, ticks):
            fresh_copy(tick).wait_send()

    for tick in range(ticks):
        for stream in range(4):
            @pl.when(exchanged(tick, stream))
            def _():
                exchange(tick, stream).wait_send()
    for tick in range(ticks - 1):
        for side in range(2):
            shift(tick, 0, side).wait_send()
            shift(tick, 3, side).wait_send()

        @pl.when(s != sections - 1)
        def _():
            for side in range(2):
                shift(tick, 1, side).wait_send()

        @pl.when(s == sections - 1)
        def _():
            finish_copy(tick).wait_send()

        @pl.when(s != 0)
        def _():
            for side in range(2):
                shift(tick, 2, side).wait_send()


def grads_kernel(
    grad_scale, stash_in, gain_in, normed_in, down_in, vals_in, up_in,
    stash_hbm, value_hbm, out_hbm, gain_hbm,
    stash, gain, normed, down, vals, up, value_grad, out_grad,
    load_sem, chunk_sem, small_sem, grad_sem,
):
    width = normed.shape[2]
    size = CHUNK if width % CHUNK == 0 else width
    count = width // size
    loads = [
        pltpu.make_async_copy(source, target, load_sem.at[index])
        for index, (source, target) in enumerate(
            ((down_in, down), (vals_in, vals), (stash_in, stash), (gain_in, gain))
        )
    ]

    def place(index):
        return pl.ds(pl.multiple_of(index * size, size), size)

    def chunks(index):
        at = place(index)
        return [
            pltpu.make_async_copy(source.at[:, :, at], target.at[:, :, at], chunk_sem.at[index, side])
            for side, (source, target) in enumerate(((normed_in, normed), (up_in, up)))
        ]

    for copy in loads[:2]:
        copy.start()
    for index in range(count):
        for copy in chunks(index):
            copy.start()
    for copy in loads[2:]:
        copy.start()
    for copy in loads[:2]:
        copy.wait()

    def step(index, _):
        at = place(index)
        for copy in chunks(index):
            copy.wait()
        for group in range(2):
            value_grad[group, at, :] = (
                transposed_times(normed[group, :, at], down[group]) * grad_scale
            ).astype(jnp.bfloat16)
            pltpu.make_async_copy(
                value_grad.at[group, at, :], value_hbm.at[group, at, :], grad_sem.at[0]
            ).start()
            out_grad[group, :, at] = (
                transposed_times(vals[group], up[group, :, at]) * grad_scale
            ).astype(jnp.bfloat16)
            pltpu.make_async_copy(
                out_grad.at[group, :, at], out_hbm.at[group, :, at], grad_sem.at[1]
            ).start()
        return None

    lax.fori_loop(0, count, step, None)
    small = [
        pltpu.make_async_copy(stash, stash_hbm, small_sem.at[0]),
        pltpu.make_async_copy(gain, gain_hbm, small_sem.at[1]),
    ]
    for load, copy in zip(loads[2:], small):
        load.wait()
        copy.start()
    pltpu.make_async_copy(value_grad, value_hbm, grad_sem.at[0]).wait()
    pltpu.make_async_copy(out_grad, out_hbm, grad_sem.at[1]).wait()
    for copy in small:
        copy.wait()


def final_kernel(own_ref, sent_ref, input_ref, cot_ref, scaled_ref, root_ref, gain_ref, activ_ref, cotan_ref):
    for group in range(2):
        total = own_ref[group].astype(jnp.float32) + sent_ref[group].astype(jnp.float32)
        activ_ref[group] = (input_ref[group].astype(jnp.float32) + total).astype(jnp.bfloat16)
        pulled = own_ref[2 + group].astype(jnp.float32) + sent_ref[2 + group].astype(jnp.float32)
        cotan_ref[group] = input_gradient(
            pulled, cot_ref[group], scaled_ref[group], root_ref[group], gain_ref[pl.ds(group, 1), :]
        )


def relay_body(
    sections,
    w_value,
    w_out,
    norm_gain,
    saved_inputs,
    arriving,
    returning,
    fresh_rows,
    targets,
    fill_slots,
    read_slots,
):
    value_mats, out_mats, gains = w_value[0], w_out[0], norm_gain[0]
    saved, activations, cotangents = saved_inputs[0], arriving[0], returning[0]
    ticks, half, width = fresh_rows.shape
    features = value_mats.shape[2]
    slots = saved.shape[0]
    if slots < 2:
        return body(
            w_value, w_out, norm_gain, saved_inputs, arriving,
            returning, fresh_rows, targets, fill_slots, read_slots,
        )
    rows = 2 * half
    vmem = pl.BlockSpec(memory_space=pltpu.VMEM)
    smem = pl.BlockSpec(memory_space=pltpu.SMEM)
    hbm = pl.BlockSpec(memory_space=pl.ANY)
    shape = jax.ShapeDtypeStruct
    narrow = jnp.bfloat16
    part_shape = shape((4, half, width), narrow)
    (
        part_own, part_peer, inputs, last_cot, scaled, root,
        stash_rows, normed, down, values, upstream, gain_sums,
    ) = pl.pallas_call(
        functools.partial(relay_kernel, sections),
        out_shape=(
            part_shape,
            part_shape,
            shape(activations.shape, narrow),
            shape(cotangents.shape, narrow),
            shape((2, half, width), jnp.float32),
            shape((2, half, 128), jnp.float32),
            shape(saved.shape, narrow),
            shape((2, ticks, 2, half, width), narrow),
            shape((2, ticks, rows, features), narrow),
            shape((2, ticks * rows, features), narrow),
            shape((2, ticks, rows, width), narrow),
            shape(gains.shape, jnp.float32),
        ),
        in_specs=[hbm, hbm, vmem] + [hbm] * 5 + [smem] * 2,
        out_specs=(hbm,) * 12,
        scratch_shapes=[
            pltpu.VMEM(saved.shape, narrow),
            pltpu.VMEM((2, ticks, 2, half, width), narrow),
            pltpu.VMEM((2, ticks, rows, features), narrow),
            pltpu.VMEM((2, ticks * rows, features), narrow),
            pltpu.VMEM((2, ticks, rows, width), narrow),
            pltpu.VMEM((ticks, half, width), narrow),
            pltpu.VMEM(value_mats.shape, narrow),
            pltpu.VMEM(out_mats.shape, narrow),
            pltpu.VMEM((ticks, 3, 2, half, width), narrow),
            pltpu.VMEM((ticks, 2, 2, half, width), narrow),
            pltpu.VMEM((slots - 1, 2, half, width), narrow),
            pltpu.VMEM((slots - 1, 2, half, width), narrow),
            pltpu.VMEM((slots, 2, half, width), narrow),
            pltpu.VMEM((ticks, 4, 2, half, width), narrow),
            pltpu.VMEM((ticks, 4, half, width), narrow),
            pltpu.VMEM((ticks, 4, half, width), narrow),
            pltpu.VMEM((rows, width), narrow),
            pltpu.VMEM((2, half, width), jnp.float32),
            pltpu.VMEM((2, half, 128), jnp.float32),
            pltpu.VMEM((2, half, width), jnp.float32),
            pltpu.VMEM((2, width), jnp.float32),
            pltpu.VMEM((2, width), jnp.float32),
            pltpu.SemaphoreType.DMA((2, 2)),
            pltpu.SemaphoreType.DMA((7,)),
            pltpu.SemaphoreType.DMA((14,)),
            pltpu.SemaphoreType.DMA((ticks, 4)),
            pltpu.SemaphoreType.DMA((ticks, 4)),
            pltpu.SemaphoreType.DMA((ticks, 4, 2)),
            pltpu.SemaphoreType.DMA((ticks, 4, 2)),
            pltpu.SemaphoreType.DMA((slots - 1, 2)),
            pltpu.SemaphoreType.DMA((slots - 1, 2)),
            pltpu.SemaphoreType.DMA((ticks,)),
            pltpu.SemaphoreType.DMA((ticks,)),
        ],
        compiler_params=pltpu.CompilerParams(
            collective_id=0, has_side_effects=True, vmem_limit_bytes=VMEM_GRANT
        ),
    )(
        value_mats, out_mats, gains, saved, activations, cotangents,
        fresh_rows, targets, fill_slots[0].T, read_slots[0].T,
    )
    part_sent = shifted(part_peer, "dp", 1)
    flat = lambda block: block.reshape(2, ticks * rows, block.shape[-1])
    operands = (stash_rows, gain_sums, flat(normed), flat(down), values, flat(upstream))
    stash_out, value_grad, out_grad, gain_grad = pl.pallas_call(
        functools.partial(grads_kernel, (ticks * rows) ** (-0.5)),
        out_shape=(
            shape(saved.shape, narrow),
            shape(value_mats.shape, narrow),
            shape(out_mats.shape, narrow),
            shape(gains.shape, jnp.float32),
        ),
        in_specs=[hbm] * 6,
        out_specs=(hbm,) * 4,
        scratch_shapes=[pltpu.VMEM(block.shape, block.dtype) for block in operands] + [
            pltpu.VMEM(value_mats.shape, narrow),
            pltpu.VMEM(out_mats.shape, narrow),
            pltpu.SemaphoreType.DMA((4,)),
            pltpu.SemaphoreType.DMA((width // CHUNK if width % CHUNK == 0 else 1, 2)),
            pltpu.SemaphoreType.DMA((2,)),
            pltpu.SemaphoreType.DMA((2,)),
        ],
        compiler_params=pltpu.CompilerParams(vmem_limit_bytes=VMEM_GRANT),
        cost_estimate=pl.CostEstimate(
            flops=32 * ticks * rows * width * features, bytes_accessed=8 * width * features, transcendentals=0
        ),
    )(*operands)
    final_rows, gradients = pl.pallas_call(
        final_kernel,
        out_shape=(shape(activations.shape, narrow), shape(cotangents.shape, narrow)),
        in_specs=[vmem] * 7,
        out_specs=(vmem,) * 2,
    )(part_own, part_sent, inputs, last_cot, scaled, root, gains)
    results = (final_rows, gradients, stash_out, value_grad, out_grad, gain_grad)
    return tuple(block[None] for block in results)


def solution(mesh):
    in_specs = (
        P("section", None, None, "dp"),
        P("section", None, "dp", None),
        P("section", None, None),
        P("section", None, None, "dp", None),
        P("section", None, "dp", None),
        P("section", None, "dp", None),
        P(None, "dp", None),
        P(None, "dp", None),
        P("section", None, None),
        P("section", None, None),
    )
    out_specs = (
        P("section", None, "dp", None),
        P("section", None, "dp", None),
        P("section", None, None, "dp", None),
        P("section", None, None, "dp"),
        P("section", None, "dp", None),
        P("section", None, None),
    )
    paired = mesh.shape["dp"] == 2 and mesh.shape["section"] > 2
    program = functools.partial(relay_body, mesh.shape["section"]) if paired else body
    return jax.shard_map(program, mesh=mesh, in_specs=in_specs, out_specs=out_specs, check_vma=False)
```

```python
import functools

import jax
import jax.numpy as jnp
from jax import lax
from jax.experimental import pallas as pl
from jax.experimental.pallas import tpu as pltpu
from jax.sharding import PartitionSpec as P

epsilon = 1e-06


def shifted(shard, axis, by):
    devices = lax.axis_size(axis)
    return lax.ppermute(shard, axis, [(i, (i + by) % devices) for i in range(devices)])


def normalize(block_rows, gain_row):
    values = block_rows.astype(jnp.float32)
    inv_root = lax.rsqrt(jnp.mean(values * values, axis=-1, keepdims=True) + epsilon)
    scaled = values * inv_root
    return (scaled, inv_root, (scaled * gain_row).astype(jnp.bfloat16))


def times_transposed(left, right):
    return lax.dot_general(
        left, right, (((1,), (1,)), ((), ())), preferred_element_type=jnp.float32
    )


def transposed_times(left, right):
    return lax.dot_general(
        left, right, (((0,), (0,)), ((), ())), preferred_element_type=jnp.float32
    )


def weight_terms(value_group, normed_all, down_grad, upstream_all):
    values = jnp.dot(normed_all, value_group, preferred_element_type=jnp.float32).astype(
        jnp.bfloat16
    )
    return (transposed_times(normed_all, down_grad), transposed_times(values, upstream_all))


def body(
    w_value,
    w_out,
    norm_gain,
    saved_inputs,
    arriving,
    returning,
    fresh_rows,
    targets,
    fill_slots,
    read_slots,
):
    value_mats = w_value[0]
    out_mats = w_out[0]
    gains = norm_gain[0]
    saved = saved_inputs[0]
    activations = arriving[0]
    cotangents = returning[0]
    tick_count = fresh_rows.shape[0]
    tok_rows = activations.shape[1]
    all_rows = tok_rows * lax.axis_size("dp")
    section_index = lax.axis_index("section")
    last_section = lax.axis_size("section") - 1
    row_offset = lax.axis_index("dp") * tok_rows
    activations, new_rows = (
        lax.all_gather(activations, "dp", axis=1, tiled=True),
        lax.all_gather(fresh_rows, "dp", axis=1, tiled=True),
    )

    def own_rows(block):
        return lax.dynamic_slice_in_dim(block, row_offset, tok_rows, 0)

    def forward(block, group):
        scaled, inv_root, normed = normalize(block, gains[group])
        values = jnp.dot(normed, value_mats[group], preferred_element_type=jnp.float32).astype(
            jnp.bfloat16
        )
        summed = lax.psum(
            jnp.dot(values, out_mats[group], preferred_element_type=jnp.float32).astype(
                jnp.bfloat16
            ),
            "dp",
        ).astype(jnp.float32)
        return (block.astype(jnp.float32) + summed).astype(jnp.bfloat16)

    value_sums = [jnp.zeros(value_mats.shape[1:], jnp.float32) for group in range(2)]
    out_sums = [jnp.zeros(out_mats.shape[1:], jnp.float32) for group in range(2)]
    gain_sums = [jnp.zeros(gains.shape[1:], jnp.float32) for group in range(2)]
    outputs = activations
    gradients = cotangents
    for tick_index in range(tick_count):
        if tick_index > 0:
            received = shifted(outputs, "section", 1)
            lower_group = jnp.where(section_index == 0, new_rows[tick_index], received[0])
            upper_group = jnp.where(section_index == 0, received[0], received[1])
            activations = jnp.stack([lower_group, upper_group])
            returned = shifted(gradients, "section", -1)
            finish = (
                own_rows(outputs[1]).astype(jnp.float32)
                - targets[tick_index - 1].astype(jnp.float32)
            ).astype(jnp.bfloat16)
            cotangents = jnp.stack(
                [
                    jnp.where(section_index == last_section, returned[1], returned[0]),
                    jnp.where(section_index == last_section, finish, returned[1]),
                ]
            )
        for group in range(2):
            saved = saved.at[fill_slots[0, tick_index, group], group].set(
                own_rows(activations[group])
            )
        outputs = jnp.stack([forward(activations[0], 0), forward(activations[1], 1)])
        fresh_grads = []
        for group in range(2):
            source = saved[read_slots[0, tick_index, group], group]
            scaled, inv_root, normed = normalize(source, gains[group])
            normed_all, upstream_all = (
                lax.all_gather(normed, "dp", axis=0, tiled=True),
                lax.all_gather(cotangents[group], "dp", axis=0, tiled=True),
            )
            down_grad = times_transposed(upstream_all, out_mats[group]).astype(jnp.bfloat16)
            pulled = lax.psum_scatter(
                times_transposed(down_grad, value_mats[group]).astype(jnp.bfloat16),
                "dp",
                scatter_dimension=0,
                tiled=True,
            ).astype(jnp.float32)
            weighted = pulled * gains[group]
            inner_mean = jnp.mean(weighted * scaled, axis=-1, keepdims=True)
            fresh_grads.append(
                (
                    cotangents[group].astype(jnp.float32)
                    + inv_root * (weighted - scaled * inner_mean)
                ).astype(jnp.bfloat16)
            )
            gain_sums[group] = gain_sums[group] + jnp.sum(pulled * scaled, axis=0)
            value_term, out_term = weight_terms(
                value_mats[group], normed_all, down_grad, upstream_all
            )
            value_sums[group] = value_sums[group] + value_term
            out_sums[group] = out_sums[group] + out_term
        gradients = jnp.stack(fresh_grads)
    grad_scale = (tick_count * all_rows) ** (-0.5)
    gain_total = lax.psum(jnp.stack(gain_sums).astype(jnp.bfloat16), "dp").astype(jnp.float32)
    final_rows = jnp.stack([own_rows(outputs[0]), own_rows(outputs[1])])
    return (
        final_rows[None],
        gradients[None],
        saved[None],
        (jnp.stack(value_sums) * grad_scale).astype(jnp.bfloat16)[None],
        (jnp.stack(out_sums) * grad_scale).astype(jnp.bfloat16)[None],
        (gain_total * grad_scale)[None],
    )


CHUNK = 512
VMEM_GRANT = 60 * 1024 * 1024
WHOLE_VMEM = 67043328
MESH = pl.DeviceIdType.MESH


def chunk_loop(width, step):
    size = CHUNK if width % CHUNK == 0 else width
    lax.fori_loop(0, width // size, lambda i, _: step(pl.ds(pl.multiple_of(i * size, size), size)), None, unroll=UNROLL)


UNROLL = 9


def contract_sum(width, term, shape):
    size = CHUNK if width % CHUNK == 0 else width

    def step(i, total):
        return total + term(pl.ds(pl.multiple_of(i * size, size), size))

    return lax.fori_loop(0, width // size, step, jnp.zeros(shape, jnp.float32), unroll=UNROLL)


def input_gradient(pulled, cotangent, scaled, root, gain_row):
    weighted = pulled * gain_row
    inner_mean = jnp.mean(weighted * scaled, axis=-1, keepdims=True)
    return (
        cotangent.astype(jnp.float32) + root[:, :1] * (weighted - scaled * inner_mean)
    ).astype(jnp.bfloat16)


def relay_kernel(
    sections,
    wv_hbm,
    wo_hbm,
    gain_ref,
    saved_hbm,
    arriving_hbm,
    returning_hbm,
    fresh_hbm,
    targets_hbm,
    fill_ref,
    read_ref,
    part_own_hbm,
    part_peer_hbm,
    input_hbm,
    cot_hbm,
    scaled_hbm,
    root_hbm,
    stash_hbm,
    normed_hbm,
    down_hbm,
    vals_hbm,
    up_hbm,
    gain_hbm,
    stash_ref,
    normed_ref,
    down_ref,
    vals_ref,
    up_ref,
    targets_ref,
    wv,
    wo,
    wv_turned,
    wo_turned,
    xin,
    cot,
    staged,
    landed,
    peer_stash,
    psend,
    precv,
    moved,
    lhs,
    scaled_own,
    root_own,
    gain_sum,
    gain_send,
    gain_recv,
    w_sem,
    in_sem,
    out_sem,
    ex_send,
    ex_recv,
    sh_send,
    sh_recv,
    st_send,
    st_recv,
    side_send,
    side_recv,
    gain_sems,
):
    s = lax.axis_index("section")
    d = lax.axis_index("dp")
    peer = 1 - d
    after = lax.rem(s + 1, sections)
    before = lax.rem(s + sections - 1, sections)
    is_last = s // (sections - 1)
    is_first = before // (sections - 1)
    ticks = fresh_hbm.shape[0]
    half, width = arriving_hbm.shape[1:]
    rows = 2 * half
    features = wv.shape[2]
    slots = saved_hbm.shape[0]

    barrier = pltpu.get_barrier_semaphore()
    for target in ((s, peer), (after, d), (before, d), (after, peer), (before, peer)):
        pl.semaphore_signal(barrier, inc=1, device_id=target, device_id_type=MESH)

    def take(index, source, target):
        copy = pltpu.make_async_copy(source, target, in_sem.at[index])
        copy.start()
        return copy

    own_blocks = {}
    for stream in (0, 3, 1, 2):
        source, buffer = (arriving_hbm, xin) if stream < 2 else (returning_hbm, cot)
        own_blocks[stream] = take(stream, source.at[stream % 2], buffer.at[0, stream % 2, 0])

    weight_copies = {}
    for group in range(2):
        for index, (source, target) in enumerate(((wv_hbm, wv), (wo_hbm, wo))):
            weight_copies[group, index] = pltpu.make_async_copy(
                source.at[group], target.at[group], w_sem.at[group, index]
            )
    for key in ((0, 0), (0, 1), (1, 1), (1, 0)):
        weight_copies[key].start()

    own_fresh = take(4, fresh_hbm.at[pl.ds(1, ticks - 1)], xin.at[pl.ds(1, ticks - 1), 2, 0])
    own_targets = take(5, targets_hbm, targets_ref)
    own_stash = take(6, saved_hbm, stash_ref)
    gain_sum[...] = jnp.zeros_like(gain_sum)
    pl.semaphore_wait(barrier, 5)

    def remote(src, dst, send, recv, target):
        return pltpu.make_async_remote_copy(
            src_ref=src, dst_ref=dst, send_sem=send, recv_sem=recv,
            device_id=target, device_id_type=MESH,
        )

    def initial(stream):
        group = stream % 2
        buffer = xin if stream < 2 else cot
        return remote(
            buffer.at[0, group, 0], buffer.at[0, group, 1],
            sh_send.at[0, stream, 1], sh_recv.at[0, stream, 1], (s, peer),
        )

    def stash_copy(index, group):
        return remote(
            staged.at[index, group], landed.at[index, group],
            st_send.at[index, group], st_recv.at[index, group], (s, peer),
        )

    def fresh_copy(tick):
        return remote(
            xin.at[tick, 2, 0], xin.at[tick, 2, 1],
            side_send.at[tick], side_recv.at[tick], (s, peer),
        )

    def gain_copy(group):
        return remote(
            gain_send.at[group], gain_recv.at[group],
            gain_sems.at[group, 0], gain_sems.at[group, 1], (s, peer),
        )

    for stream in (0, 3, 1, 2):
        own_blocks[stream].wait()
        initial(stream).start()
    own_fresh.wait()
    own_targets.wait()

    def whole(block):
        return block.astype(jnp.float32).reshape(rows, block.shape[2])

    def parted(block):
        return block.reshape(2, half, block.shape[1]).astype(jnp.bfloat16)

    def exchange(tick, stream):
        return remote(
            psend.at[tick, stream, 1], precv.at[tick, stream],
            ex_send.at[tick, stream], ex_recv.at[tick, stream], (s, peer),
        )

    def shift(tick, stream, side):
        group = stream % 2
        if stream < 2:
            place, target, buffer = (group + is_last) % 2, after, xin
        else:
            place, target, buffer = (group + is_first) % 2, before, cot
        return remote(
            moved.at[tick, stream], buffer.at[tick + 1, place, side],
            sh_send.at[tick + 1, stream, side], sh_recv.at[tick + 1, stream - group + place, side],
            (target, peer if side else d),
        )

    def finish_copy(tick):
        return remote(
            cot.at[tick + 1, 1, 0], cot.at[tick + 1, 1, 1],
            sh_send.at[tick + 1, 1, 1], sh_recv.at[tick + 1, 3, 1], (s, peer),
        )

    def arrival(tick, stream, side):
        buffer = xin if stream < 2 else cot
        return remote(
            moved.at[0, stream], buffer.at[tick, stream % 2, side],
            sh_send.at[tick, stream, side], sh_recv.at[tick, stream, side], (s, peer),
        )

    def arrive(tick, stream):
        later = tick > 0
        if stream == 0:
            near, far = later & (s != 0), (tick == 0) | (s != 0)
        elif stream == 3:
            near, far = later & (s != sections - 1), None
        else:
            near, far = later, None

        @pl.when(near)
        def _():
            arrival(tick, stream, 0).wait_recv()

        if far is None:
            arrival(tick, stream, 1).wait_recv()
        else:
            @pl.when(far)
            def _():
                arrival(tick, stream, 1).wait_recv()

            @pl.when(later & (s == 0))
            def _():
                fresh_copy(tick).wait_recv()

    def input_place(tick, group):
        return 2 * is_first * jnp.minimum(tick, 1) if group == 0 else 1

    def norm_parts(values, group):
        inv_root = lax.rsqrt(jnp.mean(values * values, axis=-1, keepdims=True) + epsilon)
        scaled = values * inv_root
        return scaled, inv_root, (scaled * gain_ref[pl.ds(group, 1), :]).astype(jnp.bfloat16)

    def weights_ready(tick, key):
        @pl.when(tick == 0)
        def _():
            weight_copies[key].wait()

    def exchanged(tick, stream):
        going = tick < ticks - 1
        return going & (s != 0) if stream == 2 else going

    def forward_start(tick, group):
        arrive(tick, group)
        lhs[...] = norm_parts(whole(xin[tick, input_place(tick, group)]), group)[2]
        if group == 0:
            weights_ready(tick, (0, 0))
        values = contract_sum(
            width,
            lambda at: jnp.dot(lhs[:, at], wv[group, at, :], preferred_element_type=jnp.float32),
            (rows, features),
        ).astype(jnp.bfloat16)
        if group == 0:
            weights_ready(tick, (0, 1))

        def step(at):
            psend[tick, group, :, :, at] = parted(
                jnp.dot(values, wo[group, :, at], preferred_element_type=jnp.float32)
            )

        chunk_loop(width, step)

        @pl.when(exchanged(tick, group))
        def _():
            exchange(tick, group).start()

    def peer_sum(tick, stream):
        exchange(tick, stream).wait_recv()
        return psend[tick, stream, 0].astype(jnp.float32) + precv[tick, stream].astype(jnp.float32)

    def forward_finish(tick, group):
        @pl.when(exchanged(tick, group))
        def _():
            own = xin[tick, input_place(tick, group), 0].astype(jnp.float32)
            outputs = (own + peer_sum(tick, group)).astype(jnp.bfloat16)
            moved[tick, group] = outputs

            def send_on():
                shift(tick, group, 1).start()
                shift(tick, group, 0).start()

            if group == 0:
                send_on()
            else:
                pl.when(s != sections - 1)(send_on)

                @pl.when(s == sections - 1)
                def _():
                    cot[tick + 1, 1, 0] = (
                        outputs.astype(jnp.float32) - targets_ref[tick].astype(jnp.float32)
                    ).astype(jnp.bfloat16)
                    finish_copy(tick).start()

    def backward_start(tick, group):
        arrive(tick, 2 + group)
        up_ref[group, tick] = whole(cot[tick, group]).astype(jnp.bfloat16)
        if group == 1:
            weights_ready(tick, (1, 1))
            weights_ready(tick, (1, 0))

        def products(out_turned, value_turned):
            down = contract_sum(
                width,
                lambda at: jnp.dot(
                    up_ref[group, tick, :, at], out_turned(at), preferred_element_type=jnp.float32
                ),
                (rows, features),
            ).astype(jnp.bfloat16)
            down_ref[group, tick] = down

            def step(at):
                psend[tick, 2 + group, :, :, at] = parted(
                    jnp.dot(down, value_turned(at), preferred_element_type=jnp.float32)
                )

            chunk_loop(width, step)

        def turn_out(at):
            turned = wo[group, :, at].T
            wo_turned[group, at, :] = turned
            return turned

        def turn_value(at):
            turned = wv[group, at, :].T
            wv_turned[group, :, at] = turned
            return turned

        @pl.when(tick == 0)
        def _():
            products(turn_out, turn_value)

        @pl.when(tick > 0)
        def _():
            products(lambda at: wo_turned[group, at, :], lambda at: wv_turned[group, :, at])

        @pl.when(exchanged(tick, 2 + group))
        def _():
            exchange(tick, 2 + group).start()

        if group == 1:
            @pl.when((tick < ticks - 1) & (s == 0))
            def _():
                fresh_copy(tick + 1).start()

    def own_source(tick, group):
        @pl.when(tick == 0)
        def _():
            if group == 1:
                own_stash.wait()
            for index in range(slots - 1):
                staged[index, group] = jnp.where(
                    fill_ref[group, 0] <= index, stash_ref[index + 1, group], stash_ref[index, group]
                )

        block = xin[tick, input_place(tick, group), 0]
        for slot in range(slots):
            stash_ref[slot, group] = jnp.where(fill_ref[group, tick] == slot, block, stash_ref[slot, group])
        source = stash_ref[read_ref[group, tick], group].astype(jnp.float32)
        scaled, inv_root, normed = norm_parts(source, group)
        normed_ref[group, tick, 0] = normed
        scaled_own[group] = scaled
        root_own[group] = jnp.broadcast_to(inv_root, root_own.shape[1:])
        gain_sum[group] += psend[tick, 2 + group, 0].astype(jnp.float32) * scaled

    def peer_stash_start(group):
        filled = fill_ref[group, 0]
        for index in range(slots - 1):
            stash_copy(index, group).wait_recv()
        for slot in range(slots):
            low, high = max(slot - 1, 0), min(slot, slots - 2)
            peer_stash[slot, group] = jnp.where(filled < slot, landed[low, group], landed[high, group])

    def peer_source(tick, group):
        block = xin[tick, input_place(tick, group), 1]
        for slot in range(slots):
            peer_stash[slot, group] = jnp.where(
                fill_ref[group, tick] == slot, block, peer_stash[slot, group]
            )
        source = peer_stash[read_ref[group, tick], group].astype(jnp.float32)
        scaled, _, normed = norm_parts(source, group)
        normed_ref[group, tick, 1] = normed
        gain_sum[group] += psend[tick, 2 + group, 1].astype(jnp.float32) * scaled

    def backward_finish(tick, group):
        @pl.when(exchanged(tick, 2 + group))
        def _():
            pulled = peer_sum(tick, 2 + group)
            moved[tick, 2 + group] = input_gradient(
                pulled, cot[tick, group, 0], scaled_own[group], root_own[group], gain_ref[pl.ds(group, 1), :]
            )
            shift(tick, 2 + group, 1).start()
            shift(tick, 2 + group, 0).start()

    def tick_step(tick, _):
        forward_start(tick, 0)
        backward_start(tick, 1)

        @pl.when(tick > 0)
        def _():
            backward_finish(tick - 1, 0)

        forward_finish(tick, 0)
        forward_start(tick, 1)
        own_source(tick, 1)
        backward_finish(tick, 1)
        backward_start(tick, 0)
        own_source(tick, 0)
        forward_finish(tick, 1)
        return None

    last = ticks - 1
    lax.fori_loop(0, last, tick_step, None)
    forward_start(last, 0)
    backward_start(last, 1)

    @pl.when(last > 0)
    def _():
        backward_finish(last - 1, 0)

    for group in (1, 0):
        for index in range(slots - 1):
            stash_copy(index, group).start()
    forward_start(last, 1)
    own_source(last, 1)
    backward_start(last, 0)
    own_source(last, 0)

    def give(index, source, target):
        copy = pltpu.make_async_copy(source, target, out_sem.at[index])
        copy.start()
        return copy

    given = [
        give(0, psend.at[last, :, 0], part_own_hbm),
        give(1, psend.at[last, :, 1], part_peer_hbm),
        give(2, xin.at[last, input_place(last, 0), 0], input_hbm.at[0]),
        give(3, xin.at[last, 1, 0], input_hbm.at[1]),
        give(4, cot.at[last, :, 0], cot_hbm),
        give(5, scaled_own, scaled_hbm),
        give(6, root_own, root_hbm),
        give(7, stash_ref, stash_hbm),
        give(8, up_ref, up_hbm),
        give(9, down_ref, down_hbm),
    ]
    for group in (1, 0):
        peer_stash_start(group)

        def source_step(tick, _):
            peer_source(tick, group)
            return None

        lax.fori_loop(0, ticks, source_step, None)
        given.append(give(10 + group, normed_ref.at[group], normed_hbm.at[group]))
        gain_send[group] = jnp.sum(gain_sum[group], axis=0, keepdims=True)
        gain_copy(group).start()

        def chunk_values(at):
            block = normed_ref[group, :, :, :, at].astype(jnp.float32)
            left = block.reshape(ticks * rows, block.shape[3]).astype(jnp.bfloat16)
            return jnp.dot(left, wv[group, at, :], preferred_element_type=jnp.float32)

        vals_ref[group] = contract_sum(width, chunk_values, (ticks * rows, features)).astype(jnp.bfloat16)
        given.append(give(12 + group, vals_ref.at[group], vals_hbm.at[group]))
    for group in (1, 0):
        gain_copy(group).wait_recv()
        gain_sum[0, pl.ds(group, 1), :] = (gain_send[group] + gain_recv[group]) * (ticks * rows) ** (-0.5)
    given.append(give(14, gain_sum.at[0, pl.ds(0, 2)], gain_hbm))
    for copy in given:
        copy.wait()

    for group in range(2):
        gain_copy(group).wait_send()
    for stream in range(4):
        initial(stream).wait_send()
    for group in range(2):
        for index in range(slots - 1):
            stash_copy(index, group).wait_send()

    @pl.when(s == 0)
    def _():
        for tick in range(1, ticks):
            fresh_copy(tick).wait_send()

    for tick in range(ticks):
        for stream in range(4):
            @pl.when(exchanged(tick, stream))
            def _():
                exchange(tick, stream).wait_send()
    for tick in range(ticks - 1):
        for side in range(2):
            shift(tick, 0, side).wait_send()
            shift(tick, 3, side).wait_send()

        @pl.when(s != sections - 1)
        def _():
            for side in range(2):
                shift(tick, 1, side).wait_send()

        @pl.when(s == sections - 1)
        def _():
            finish_copy(tick).wait_send()

        @pl.when(s != 0)
        def _():
            for side in range(2):
                shift(tick, 2, side).wait_send()


def grads_kernel(
    grad_scale, stash_in, gain_in, normed_in, down_in, vals_in, up_in,
    stash_hbm, value_hbm, out_hbm, gain_hbm,
    stash, gain, normed, down, vals, up, value_grad, out_grad,
    load_sem, chunk_sem, small_sem, grad_sem,
):
    width = normed.shape[2]
    size = CHUNK if width % CHUNK == 0 else width
    count = width // size
    loads = [
        pltpu.make_async_copy(source, target, load_sem.at[index])
        for index, (source, target) in enumerate(
            ((down_in, down), (vals_in, vals), (stash_in, stash), (gain_in, gain))
        )
    ]

    def place(index):
        return pl.ds(pl.multiple_of(index * size, size), size)

    def chunks(index):
        at = place(index)
        return [
            pltpu.make_async_copy(source.at[:, :, at], target.at[:, :, at], chunk_sem.at[index, side])
            for side, (source, target) in enumerate(((normed_in, normed), (up_in, up)))
        ]

    for copy in loads[:2]:
        copy.start()
    for index in range(count):
        for copy in chunks(index):
            copy.start()
    for copy in loads[2:]:
        copy.start()
    for copy in loads[:2]:
        copy.wait()

    def step(index, _):
        at = place(index)
        for copy in chunks(index):
            copy.wait()
        for group in range(2):
            value_grad[group, at, :] = (
                transposed_times(normed[group, :, at], down[group]) * grad_scale
            ).astype(jnp.bfloat16)
            pltpu.make_async_copy(
                value_grad.at[group, at, :], value_hbm.at[group, at, :], grad_sem.at[0]
            ).start()
            out_grad[group, :, at] = (
                transposed_times(vals[group], up[group, :, at]) * grad_scale
            ).astype(jnp.bfloat16)
            pltpu.make_async_copy(
                out_grad.at[group, :, at], out_hbm.at[group, :, at], grad_sem.at[1]
            ).start()
        return None

    lax.fori_loop(0, count, step, None)
    small = [
        pltpu.make_async_copy(stash, stash_hbm, small_sem.at[0]),
        pltpu.make_async_copy(gain, gain_hbm, small_sem.at[1]),
    ]
    for load, copy in zip(loads[2:], small):
        load.wait()
        copy.start()
    pltpu.make_async_copy(value_grad, value_hbm, grad_sem.at[0]).wait()
    pltpu.make_async_copy(out_grad, out_hbm, grad_sem.at[1]).wait()
    for copy in small:
        copy.wait()


def final_kernel(own_ref, sent_ref, input_ref, cot_ref, scaled_ref, root_ref, gain_ref, activ_ref, cotan_ref):
    for group in range(2):
        total = own_ref[group].astype(jnp.float32) + sent_ref[group].astype(jnp.float32)
        activ_ref[group] = (input_ref[group].astype(jnp.float32) + total).astype(jnp.bfloat16)
        pulled = own_ref[2 + group].astype(jnp.float32) + sent_ref[2 + group].astype(jnp.float32)
        cotan_ref[group] = input_gradient(
            pulled, cot_ref[group], scaled_ref[group], root_ref[group], gain_ref[pl.ds(group, 1), :]
        )


def relay_body(
    sections,
    w_value,
    w_out,
    norm_gain,
    saved_inputs,
    arriving,
    returning,
    fresh_rows,
    targets,
    fill_slots,
    read_slots,
):
    value_mats, out_mats, gains = w_value[0], w_out[0], norm_gain[0]
    saved, activations, cotangents = saved_inputs[0], arriving[0], returning[0]
    ticks, half, width = fresh_rows.shape
    features = value_mats.shape[2]
    slots = saved.shape[0]
    if slots < 2:
        return body(
            w_value, w_out, norm_gain, saved_inputs, arriving,
            returning, fresh_rows, targets, fill_slots, read_slots,
        )
    rows = 2 * half
    vmem = pl.BlockSpec(memory_space=pltpu.VMEM)
    smem = pl.BlockSpec(memory_space=pltpu.SMEM)
    hbm = pl.BlockSpec(memory_space=pl.ANY)
    shape = jax.ShapeDtypeStruct
    narrow = jnp.bfloat16
    part_shape = shape((4, half, width), narrow)
    (
        part_own, part_peer, inputs, last_cot, scaled, root,
        stash_rows, normed, down, values, upstream, gain_sums,
    ) = pl.pallas_call(
        functools.partial(relay_kernel, sections),
        out_shape=(
            part_shape,
            part_shape,
            shape(activations.shape, narrow),
            shape(cotangents.shape, narrow),
            shape((2, half, width), jnp.float32),
            shape((2, half, 128), jnp.float32),
            shape(saved.shape, narrow),
            shape((2, ticks, 2, half, width), narrow),
            shape((2, ticks, rows, features), narrow),
            shape((2, ticks * rows, features), narrow),
            shape((2, ticks, rows, width), narrow),
            shape(gains.shape, jnp.float32),
        ),
        in_specs=[hbm, hbm, vmem] + [hbm] * 5 + [smem] * 2,
        out_specs=(hbm,) * 12,
        scratch_shapes=[
            pltpu.VMEM(saved.shape, narrow),
            pltpu.VMEM((2, ticks, 2, half, width), narrow),
            pltpu.VMEM((2, ticks, rows, features), narrow),
            pltpu.VMEM((2, ticks * rows, features), narrow),
            pltpu.VMEM((2, ticks, rows, width), narrow),
            pltpu.VMEM((ticks, half, width), narrow),
            pltpu.VMEM(value_mats.shape, narrow),
            pltpu.VMEM(out_mats.shape, narrow),
            pltpu.VMEM((2, features, width), narrow),
            pltpu.VMEM((2, width, features), narrow),
            pltpu.VMEM((ticks, 3, 2, half, width), narrow),
            pltpu.VMEM((ticks, 2, 2, half, width), narrow),
            pltpu.VMEM((slots - 1, 2, half, width), narrow),
            pltpu.VMEM((slots - 1, 2, half, width), narrow),
            pltpu.VMEM((slots, 2, half, width), narrow),
            pltpu.VMEM((ticks, 4, 2, half, width), narrow),
            pltpu.VMEM((ticks, 4, half, width), narrow),
            pltpu.VMEM((ticks, 4, half, width), narrow),
            pltpu.VMEM((rows, width), narrow),
            pltpu.VMEM((2, half, width), jnp.float32),
            pltpu.VMEM((2, half, 128), jnp.float32),
            pltpu.VMEM((2, half, width), jnp.float32),
            pltpu.VMEM((2, 1, width), jnp.float32),
            pltpu.VMEM((2, 1, width), jnp.float32),
            pltpu.SemaphoreType.DMA((2, 2)),
            pltpu.SemaphoreType.DMA((7,)),
            pltpu.SemaphoreType.DMA((15,)),
            pltpu.SemaphoreType.DMA((ticks, 4)),
            pltpu.SemaphoreType.DMA((ticks, 4)),
            pltpu.SemaphoreType.DMA((ticks, 4, 2)),
            pltpu.SemaphoreType.DMA((ticks, 4, 2)),
            pltpu.SemaphoreType.DMA((slots - 1, 2)),
            pltpu.SemaphoreType.DMA((slots - 1, 2)),
            pltpu.SemaphoreType.DMA((ticks,)),
            pltpu.SemaphoreType.DMA((ticks,)),
            pltpu.SemaphoreType.DMA((2, 2)),
        ],
        compiler_params=pltpu.CompilerParams(
            collective_id=0, has_side_effects=True, vmem_limit_bytes=VMEM_GRANT
        ),
    )(
        value_mats, out_mats, gains, saved, activations, cotangents,
        fresh_rows, targets, fill_slots[0].T, read_slots[0].T,
    )
    part_sent = shifted(part_peer, "dp", 1)
    flat = lambda block: block.reshape(2, ticks * rows, block.shape[-1])
    operands = (stash_rows, gain_sums, flat(normed), flat(down), values, flat(upstream))
    stash_out, value_grad, out_grad, gain_grad = pl.pallas_call(
        functools.partial(grads_kernel, (ticks * rows) ** (-0.5)),
        out_shape=(
            shape(saved.shape, narrow),
            shape(value_mats.shape, narrow),
            shape(out_mats.shape, narrow),
            shape(gains.shape, jnp.float32),
        ),
        in_specs=[hbm] * 6,
        out_specs=(hbm,) * 4,
        scratch_shapes=[pltpu.VMEM(block.shape, block.dtype) for block in operands] + [
            pltpu.VMEM(value_mats.shape, narrow),
            pltpu.VMEM(out_mats.shape, narrow),
            pltpu.SemaphoreType.DMA((4,)),
            pltpu.SemaphoreType.DMA((width // CHUNK if width % CHUNK == 0 else 1, 2)),
            pltpu.SemaphoreType.DMA((2,)),
            pltpu.SemaphoreType.DMA((2,)),
        ],
        compiler_params=pltpu.CompilerParams(vmem_limit_bytes=WHOLE_VMEM),
        cost_estimate=pl.CostEstimate(
            flops=32 * ticks * rows * width * features, bytes_accessed=8 * width * features, transcendentals=0
        ),
    )(*operands)
    final_rows, gradients = pl.pallas_call(
        final_kernel,
        out_shape=(shape(activations.shape, narrow), shape(cotangents.shape, narrow)),
        in_specs=[vmem] * 7,
        out_specs=(vmem,) * 2,
    )(part_own, part_sent, inputs, last_cot, scaled, root, gains)
    results = (final_rows, gradients, stash_out, value_grad, out_grad, gain_grad)
    return tuple(block[None] for block in results)


def solution(mesh):
    in_specs = (
        P("section", None, None, "dp"),
        P("section", None, "dp", None),
        P("section", None, None),
        P("section", None, None, "dp", None),
        P("section", None, "dp", None),
        P("section", None, "dp", None),
        P(None, "dp", None),
        P(None, "dp", None),
        P("section", None, None),
        P("section", None, None),
    )
    out_specs = (
        P("section", None, "dp", None),
        P("section", None, "dp", None),
        P("section", None, None, "dp", None),
        P("section", None, None, "dp"),
        P("section", None, "dp", None),
        P("section", None, None),
    )
    paired = mesh.shape["dp"] == 2 and mesh.shape["section"] > 2
    program = functools.partial(relay_body, mesh.shape["section"]) if paired else body
    return jax.shard_map(program, mesh=mesh, in_specs=in_specs, out_specs=out_specs, check_vma=False)
```

```python
import functools

import jax
import jax.numpy as jnp
from jax import lax
from jax.experimental import pallas as pl
from jax.experimental.pallas import tpu as pltpu
from jax.sharding import PartitionSpec as P

epsilon = 1e-06


def shifted(shard, axis, by):
    devices = lax.axis_size(axis)
    return lax.ppermute(shard, axis, [(i, (i + by) % devices) for i in range(devices)])


def normalize(block_rows, gain_row):
    values = block_rows.astype(jnp.float32)
    inv_root = lax.rsqrt(jnp.mean(values * values, axis=-1, keepdims=True) + epsilon)
    scaled = values * inv_root
    return (scaled, inv_root, (scaled * gain_row).astype(jnp.bfloat16))


def times_transposed(left, right):
    return lax.dot_general(
        left, right, (((1,), (1,)), ((), ())), preferred_element_type=jnp.float32
    )


def transposed_times(left, right):
    return lax.dot_general(
        left, right, (((0,), (0,)), ((), ())), preferred_element_type=jnp.float32
    )


def weight_terms(value_group, normed_all, down_grad, upstream_all):
    values = jnp.dot(normed_all, value_group, preferred_element_type=jnp.float32).astype(
        jnp.bfloat16
    )
    return (transposed_times(normed_all, down_grad), transposed_times(values, upstream_all))


def body(
    w_value,
    w_out,
    norm_gain,
    saved_inputs,
    arriving,
    returning,
    fresh_rows,
    targets,
    fill_slots,
    read_slots,
):
    value_mats = w_value[0]
    out_mats = w_out[0]
    gains = norm_gain[0]
    saved = saved_inputs[0]
    activations = arriving[0]
    cotangents = returning[0]
    tick_count = fresh_rows.shape[0]
    tok_rows = activations.shape[1]
    all_rows = tok_rows * lax.axis_size("dp")
    section_index = lax.axis_index("section")
    last_section = lax.axis_size("section") - 1
    row_offset = lax.axis_index("dp") * tok_rows
    activations, new_rows = (
        lax.all_gather(activations, "dp", axis=1, tiled=True),
        lax.all_gather(fresh_rows, "dp", axis=1, tiled=True),
    )

    def own_rows(block):
        return lax.dynamic_slice_in_dim(block, row_offset, tok_rows, 0)

    def forward(block, group):
        scaled, inv_root, normed = normalize(block, gains[group])
        values = jnp.dot(normed, value_mats[group], preferred_element_type=jnp.float32).astype(
            jnp.bfloat16
        )
        summed = lax.psum(
            jnp.dot(values, out_mats[group], preferred_element_type=jnp.float32).astype(
                jnp.bfloat16
            ),
            "dp",
        ).astype(jnp.float32)
        return (block.astype(jnp.float32) + summed).astype(jnp.bfloat16)

    value_sums = [jnp.zeros(value_mats.shape[1:], jnp.float32) for group in range(2)]
    out_sums = [jnp.zeros(out_mats.shape[1:], jnp.float32) for group in range(2)]
    gain_sums = [jnp.zeros(gains.shape[1:], jnp.float32) for group in range(2)]
    outputs = activations
    gradients = cotangents
    for tick_index in range(tick_count):
        if tick_index > 0:
            received = shifted(outputs, "section", 1)
            lower_group = jnp.where(section_index == 0, new_rows[tick_index], received[0])
            upper_group = jnp.where(section_index == 0, received[0], received[1])
            activations = jnp.stack([lower_group, upper_group])
            returned = shifted(gradients, "section", -1)
            finish = (
                own_rows(outputs[1]).astype(jnp.float32)
                - targets[tick_index - 1].astype(jnp.float32)
            ).astype(jnp.bfloat16)
            cotangents = jnp.stack(
                [
                    jnp.where(section_index == last_section, returned[1], returned[0]),
                    jnp.where(section_index == last_section, finish, returned[1]),
                ]
            )
        for group in range(2):
            saved = saved.at[fill_slots[0, tick_index, group], group].set(
                own_rows(activations[group])
            )
        outputs = jnp.stack([forward(activations[0], 0), forward(activations[1], 1)])
        fresh_grads = []
        for group in range(2):
            source = saved[read_slots[0, tick_index, group], group]
            scaled, inv_root, normed = normalize(source, gains[group])
            normed_all, upstream_all = (
                lax.all_gather(normed, "dp", axis=0, tiled=True),
                lax.all_gather(cotangents[group], "dp", axis=0, tiled=True),
            )
            down_grad = times_transposed(upstream_all, out_mats[group]).astype(jnp.bfloat16)
            pulled = lax.psum_scatter(
                times_transposed(down_grad, value_mats[group]).astype(jnp.bfloat16),
                "dp",
                scatter_dimension=0,
                tiled=True,
            ).astype(jnp.float32)
            weighted = pulled * gains[group]
            inner_mean = jnp.mean(weighted * scaled, axis=-1, keepdims=True)
            fresh_grads.append(
                (
                    cotangents[group].astype(jnp.float32)
                    + inv_root * (weighted - scaled * inner_mean)
                ).astype(jnp.bfloat16)
            )
            gain_sums[group] = gain_sums[group] + jnp.sum(pulled * scaled, axis=0)
            value_term, out_term = weight_terms(
                value_mats[group], normed_all, down_grad, upstream_all
            )
            value_sums[group] = value_sums[group] + value_term
            out_sums[group] = out_sums[group] + out_term
        gradients = jnp.stack(fresh_grads)
    grad_scale = (tick_count * all_rows) ** (-0.5)
    gain_total = lax.psum(jnp.stack(gain_sums).astype(jnp.bfloat16), "dp").astype(jnp.float32)
    final_rows = jnp.stack([own_rows(outputs[0]), own_rows(outputs[1])])
    return (
        final_rows[None],
        gradients[None],
        saved[None],
        (jnp.stack(value_sums) * grad_scale).astype(jnp.bfloat16)[None],
        (jnp.stack(out_sums) * grad_scale).astype(jnp.bfloat16)[None],
        (gain_total * grad_scale)[None],
    )


CHUNK = 512
VMEM_GRANT = 60 * 1024 * 1024
WHOLE_VMEM = 67043328
MESH = pl.DeviceIdType.MESH


def chunk_loop(width, step):
    size = CHUNK if width % CHUNK == 0 else width
    lax.fori_loop(0, width // size, lambda i, _: step(pl.ds(pl.multiple_of(i * size, size), size)), None, unroll=UNROLL)


UNROLL = 9


def contract_sum(width, term, shape):
    size = CHUNK if width % CHUNK == 0 else width

    def step(i, total):
        return total + term(pl.ds(pl.multiple_of(i * size, size), size))

    return lax.fori_loop(0, width // size, step, jnp.zeros(shape, jnp.float32), unroll=UNROLL)


def input_gradient(pulled, cotangent, scaled, root, gain_row):
    weighted = pulled * gain_row
    inner_mean = jnp.mean(weighted * scaled, axis=-1, keepdims=True)
    return (
        cotangent.astype(jnp.float32) + root[:, :1] * (weighted - scaled * inner_mean)
    ).astype(jnp.bfloat16)


def relay_kernel(
    sections,
    wv_hbm,
    wo_hbm,
    gain_ref,
    saved_hbm,
    arriving_hbm,
    returning_hbm,
    fresh_hbm,
    targets_hbm,
    fill_ref,
    read_ref,
    part_own_hbm,
    part_peer_hbm,
    input_hbm,
    cot_hbm,
    scaled_hbm,
    root_hbm,
    stash_hbm,
    normed_hbm,
    down_hbm,
    vals_hbm,
    up_hbm,
    gain_hbm,
    stash_ref,
    normed_ref,
    down_ref,
    vals_ref,
    up_ref,
    targets_ref,
    wv,
    wo,
    wv_turned,
    wo_turned,
    xin,
    cot,
    staged,
    landed,
    peer_stash,
    psend,
    precv,
    moved,
    lhs,
    scaled_own,
    root_own,
    gain_sum,
    gain_send,
    gain_recv,
    w_sem,
    in_sem,
    out_sem,
    ex_send,
    ex_recv,
    sh_send,
    sh_recv,
    st_send,
    st_recv,
    side_send,
    side_recv,
    gain_sems,
):
    s = lax.axis_index("section")
    d = lax.axis_index("dp")
    peer = 1 - d
    after = lax.rem(s + 1, sections)
    before = lax.rem(s + sections - 1, sections)
    is_last = s // (sections - 1)
    is_first = before // (sections - 1)
    ticks = fresh_hbm.shape[0]
    half, width = arriving_hbm.shape[1:]
    rows = 2 * half
    features = wv.shape[2]
    slots = saved_hbm.shape[0]

    barrier = pltpu.get_barrier_semaphore()
    for target in ((s, peer), (after, d), (before, d), (after, peer), (before, peer)):
        pl.semaphore_signal(barrier, inc=1, device_id=target, device_id_type=MESH)

    def take(index, source, target):
        copy = pltpu.make_async_copy(source, target, in_sem.at[index])
        copy.start()
        return copy

    own_blocks = {}
    for stream in (0, 3, 1, 2):
        source, buffer = (arriving_hbm, xin) if stream < 2 else (returning_hbm, cot)
        own_blocks[stream] = take(stream, source.at[stream % 2], buffer.at[0, stream % 2, 0])

    weight_copies = {}
    for group in range(2):
        for index, (source, target) in enumerate(((wv_hbm, wv), (wo_hbm, wo))):
            weight_copies[group, index] = pltpu.make_async_copy(
                source.at[group], target.at[group], w_sem.at[group, index]
            )
    for key in ((0, 0), (0, 1), (1, 1), (1, 0)):
        weight_copies[key].start()

    own_fresh = take(4, fresh_hbm.at[pl.ds(1, ticks - 1)], xin.at[pl.ds(1, ticks - 1), 2, 0])
    own_targets = take(5, targets_hbm, targets_ref)
    own_stash = take(6, saved_hbm, stash_ref)
    gain_sum[...] = jnp.zeros_like(gain_sum)
    pl.semaphore_wait(barrier, 5)

    def remote(src, dst, send, recv, target):
        return pltpu.make_async_remote_copy(
            src_ref=src, dst_ref=dst, send_sem=send, recv_sem=recv,
            device_id=target, device_id_type=MESH,
        )

    def initial(stream):
        group = stream % 2
        buffer = xin if stream < 2 else cot
        return remote(
            buffer.at[0, group, 0], buffer.at[0, group, 1],
            sh_send.at[0, stream, 1], sh_recv.at[0, stream, 1], (s, peer),
        )

    def stash_copy(index, group):
        return remote(
            staged.at[index, group], landed.at[index, group],
            st_send.at[index, group], st_recv.at[index, group], (s, peer),
        )

    def fresh_copy(tick):
        return remote(
            xin.at[tick, 2, 0], xin.at[tick, 2, 1],
            side_send.at[tick], side_recv.at[tick], (s, peer),
        )

    def gain_copy(group):
        return remote(
            gain_send.at[group], gain_recv.at[group],
            gain_sems.at[group, 0], gain_sems.at[group, 1], (s, peer),
        )

    for stream in (0, 3, 1, 2):
        own_blocks[stream].wait()
        initial(stream).start()
    own_fresh.wait()
    own_targets.wait()

    def whole(block):
        return block.astype(jnp.float32).reshape(rows, block.shape[2])

    def parted(block):
        return block.reshape(2, half, block.shape[1]).astype(jnp.bfloat16)

    def exchange(tick, stream):
        return remote(
            psend.at[tick, stream, 1], precv.at[tick, stream],
            ex_send.at[tick, stream], ex_recv.at[tick, stream], (s, peer),
        )

    def shift(tick, stream, side):
        group = stream % 2
        if stream < 2:
            place, target, buffer = (group + is_last) % 2, after, xin
        else:
            place, target, buffer = (group + is_first) % 2, before, cot
        return remote(
            moved.at[tick, stream], buffer.at[tick + 1, place, side],
            sh_send.at[tick + 1, stream, side], sh_recv.at[tick + 1, stream - group + place, side],
            (target, peer if side else d),
        )

    def finish_copy(tick):
        return remote(
            cot.at[tick + 1, 1, 0], cot.at[tick + 1, 1, 1],
            sh_send.at[tick + 1, 1, 1], sh_recv.at[tick + 1, 3, 1], (s, peer),
        )

    def arrival(tick, stream, side):
        buffer = xin if stream < 2 else cot
        return remote(
            moved.at[0, stream], buffer.at[tick, stream % 2, side],
            sh_send.at[tick, stream, side], sh_recv.at[tick, stream, side], (s, peer),
        )

    def arrive(tick, stream):
        later = tick > 0
        if stream == 0:
            near, far = later & (s != 0), (tick == 0) | (s != 0)
        elif stream == 3:
            near, far = later & (s != sections - 1), None
        else:
            near, far = later, None

        @pl.when(near)
        def _():
            arrival(tick, stream, 0).wait_recv()

        if far is None:
            arrival(tick, stream, 1).wait_recv()
        else:
            @pl.when(far)
            def _():
                arrival(tick, stream, 1).wait_recv()

            @pl.when(later & (s == 0))
            def _():
                fresh_copy(tick).wait_recv()

    def input_place(tick, group):
        return 2 * is_first * jnp.minimum(tick, 1) if group == 0 else 1

    def norm_parts(values, group):
        inv_root = lax.rsqrt(jnp.mean(values * values, axis=-1, keepdims=True) + epsilon)
        scaled = values * inv_root
        return scaled, inv_root, (scaled * gain_ref[pl.ds(group, 1), :]).astype(jnp.bfloat16)

    def weights_ready(tick, key):
        @pl.when(tick == 0)
        def _():
            weight_copies[key].wait()

    def exchanged(tick, stream):
        going = tick < ticks - 1
        return going & (s != 0) if stream == 2 else going

    def forward_start(tick, group):
        arrive(tick, group)
        lhs[...] = norm_parts(whole(xin[tick, input_place(tick, group)]), group)[2]
        if group == 0:
            weights_ready(tick, (0, 0))
        values = contract_sum(
            width,
            lambda at: jnp.dot(lhs[:, at], wv[group, at, :], preferred_element_type=jnp.float32),
            (rows, features),
        ).astype(jnp.bfloat16)
        if group == 0:
            weights_ready(tick, (0, 1))

        def step(at):
            psend[tick, group, :, :, at] = parted(
                jnp.dot(values, wo[group, :, at], preferred_element_type=jnp.float32)
            )

        chunk_loop(width, step)

        @pl.when(exchanged(tick, group))
        def _():
            exchange(tick, group).start()

    def peer_sum(tick, stream):
        exchange(tick, stream).wait_recv()
        return psend[tick, stream, 0].astype(jnp.float32) + precv[tick, stream].astype(jnp.float32)

    def forward_finish(tick, group):
        @pl.when(exchanged(tick, group))
        def _():
            own = xin[tick, input_place(tick, group), 0].astype(jnp.float32)
            outputs = (own + peer_sum(tick, group)).astype(jnp.bfloat16)
            moved[tick, group] = outputs

            def send_on():
                shift(tick, group, 0).start()
                shift(tick, group, 1).start()

            if group == 0:
                send_on()
            else:
                pl.when(s != sections - 1)(send_on)

                @pl.when(s == sections - 1)
                def _():
                    cot[tick + 1, 1, 0] = (
                        outputs.astype(jnp.float32) - targets_ref[tick].astype(jnp.float32)
                    ).astype(jnp.bfloat16)
                    finish_copy(tick).start()

    def backward_start(tick, group):
        arrive(tick, 2 + group)
        up_ref[group, tick] = whole(cot[tick, group]).astype(jnp.bfloat16)
        if group == 1:
            weights_ready(tick, (1, 1))
            weights_ready(tick, (1, 0))

        def products(out_turned, value_turned):
            down = contract_sum(
                width,
                lambda at: jnp.dot(
                    up_ref[group, tick, :, at], out_turned(at), preferred_element_type=jnp.float32
                ),
                (rows, features),
            ).astype(jnp.bfloat16)
            down_ref[group, tick] = down

            def step(at):
                psend[tick, 2 + group, :, :, at] = parted(
                    jnp.dot(down, value_turned(at), preferred_element_type=jnp.float32)
                )

            chunk_loop(width, step)

        def turn_out(at):
            turned = wo[group, :, at].T
            wo_turned[group, at, :] = turned
            return turned

        def turn_value(at):
            turned = wv[group, at, :].T
            wv_turned[group, :, at] = turned
            return turned

        @pl.when(tick == 0)
        def _():
            products(turn_out, turn_value)

        @pl.when(tick > 0)
        def _():
            products(lambda at: wo_turned[group, at, :], lambda at: wv_turned[group, :, at])

        @pl.when(exchanged(tick, 2 + group))
        def _():
            exchange(tick, 2 + group).start()

        if group == 1:
            @pl.when((tick < ticks - 1) & (s == 0))
            def _():
                fresh_copy(tick + 1).start()

    def own_source(tick, group):
        @pl.when(tick == 0)
        def _():
            if group == 1:
                own_stash.wait()
            for index in range(slots - 1):
                staged[index, group] = jnp.where(
                    fill_ref[group, 0] <= index, stash_ref[index + 1, group], stash_ref[index, group]
                )

        block = xin[tick, input_place(tick, group), 0]
        for slot in range(slots):
            stash_ref[slot, group] = jnp.where(fill_ref[group, tick] == slot, block, stash_ref[slot, group])
        source = stash_ref[read_ref[group, tick], group].astype(jnp.float32)
        scaled, inv_root, normed = norm_parts(source, group)
        normed_ref[group, tick, 0] = normed
        scaled_own[group] = scaled
        root_own[group] = jnp.broadcast_to(inv_root, root_own.shape[1:])
        gain_sum[group] += psend[tick, 2 + group, 0].astype(jnp.float32) * scaled

    def peer_stash_start(group):
        filled = fill_ref[group, 0]
        for index in range(slots - 1):
            stash_copy(index, group).wait_recv()
        for slot in range(slots):
            low, high = max(slot - 1, 0), min(slot, slots - 2)
            peer_stash[slot, group] = jnp.where(filled < slot, landed[low, group], landed[high, group])

    def peer_source(tick, group):
        block = xin[tick, input_place(tick, group), 1]
        for slot in range(slots):
            peer_stash[slot, group] = jnp.where(
                fill_ref[group, tick] == slot, block, peer_stash[slot, group]
            )
        source = peer_stash[read_ref[group, tick], group].astype(jnp.float32)
        scaled, _, normed = norm_parts(source, group)
        normed_ref[group, tick, 1] = normed
        gain_sum[group] += psend[tick, 2 + group, 1].astype(jnp.float32) * scaled

    def backward_finish(tick, group):
        @pl.when(exchanged(tick, 2 + group))
        def _():
            pulled = peer_sum(tick, 2 + group)
            moved[tick, 2 + group] = input_gradient(
                pulled, cot[tick, group, 0], scaled_own[group], root_own[group], gain_ref[pl.ds(group, 1), :]
            )
            shift(tick, 2 + group, 0).start()
            shift(tick, 2 + group, 1).start()

    last = ticks - 1

    def tick_step(tick, _):
        forward_start(tick, 0)
        backward_start(tick, 1)

        @pl.when(tick > 0)
        def _():
            backward_finish(tick - 1, 0)

        forward_finish(tick, 0)
        forward_start(tick, 1)
        own_source(tick, 1)
        backward_finish(tick, 1)
        backward_start(tick, 0)
        own_source(tick, 0)
        forward_finish(tick, 1)

        @pl.when(tick == jnp.maximum(last - 1, 0))
        def _():
            for group in (1, 0):
                for index in range(slots - 1):
                    stash_copy(index, group).start()
        return None

    lax.fori_loop(0, last, tick_step, None)
    forward_start(last, 0)
    backward_start(last, 1)

    @pl.when(last > 0)
    def _():
        backward_finish(last - 1, 0)

    forward_start(last, 1)
    own_source(last, 1)
    backward_start(last, 0)
    own_source(last, 0)

    def give(index, source, target):
        copy = pltpu.make_async_copy(source, target, out_sem.at[index])
        copy.start()
        return copy

    given = [
        give(0, psend.at[last, :, 0], part_own_hbm),
        give(1, psend.at[last, :, 1], part_peer_hbm),
        give(2, xin.at[last, input_place(last, 0), 0], input_hbm.at[0]),
        give(3, xin.at[last, 1, 0], input_hbm.at[1]),
        give(4, cot.at[last, :, 0], cot_hbm),
        give(5, scaled_own, scaled_hbm),
        give(6, root_own, root_hbm),
        give(7, stash_ref, stash_hbm),
        give(8, up_ref, up_hbm),
        give(9, down_ref, down_hbm),
    ]
    for group in (1, 0):
        peer_stash_start(group)

        def source_step(tick, _):
            peer_source(tick, group)
            return None

        lax.fori_loop(0, ticks, source_step, None)
        given.append(give(10 + group, normed_ref.at[group], normed_hbm.at[group]))
        gain_send[group] = jnp.sum(gain_sum[group], axis=0, keepdims=True)
        gain_copy(group).start()

        def chunk_values(at):
            block = normed_ref[group, :, :, :, at].astype(jnp.float32)
            left = block.reshape(ticks * rows, block.shape[3]).astype(jnp.bfloat16)
            return jnp.dot(left, wv[group, at, :], preferred_element_type=jnp.float32)

        vals_ref[group] = contract_sum(width, chunk_values, (ticks * rows, features)).astype(jnp.bfloat16)
        given.append(give(12 + group, vals_ref.at[group], vals_hbm.at[group]))
    for group in (1, 0):
        gain_copy(group).wait_recv()
        gain_sum[0, pl.ds(group, 1), :] = (gain_send[group] + gain_recv[group]) * (ticks * rows) ** (-0.5)
    given.append(give(14, gain_sum.at[0, pl.ds(0, 2)], gain_hbm))
    for copy in given:
        copy.wait()

    for group in range(2):
        gain_copy(group).wait_send()
    for stream in range(4):
        initial(stream).wait_send()
    for group in range(2):
        for index in range(slots - 1):
            stash_copy(index, group).wait_send()

    @pl.when(s == 0)
    def _():
        for tick in range(1, ticks):
            fresh_copy(tick).wait_send()

    for tick in range(ticks):
        for stream in range(4):
            @pl.when(exchanged(tick, stream))
            def _():
                exchange(tick, stream).wait_send()
    for tick in range(ticks - 1):
        for side in range(2):
            shift(tick, 0, side).wait_send()
            shift(tick, 3, side).wait_send()

        @pl.when(s != sections - 1)
        def _():
            for side in range(2):
                shift(tick, 1, side).wait_send()

        @pl.when(s == sections - 1)
        def _():
            finish_copy(tick).wait_send()

        @pl.when(s != 0)
        def _():
            for side in range(2):
                shift(tick, 2, side).wait_send()


def grads_kernel(
    grad_scale, stash_in, gain_in, normed_in, down_in, vals_in, up_in,
    stash_hbm, value_hbm, out_hbm, gain_hbm,
    stash, gain, normed, down, vals, up, value_grad, out_grad,
    load_sem, chunk_sem, small_sem, grad_sem,
):
    width = normed.shape[2]
    size = CHUNK if width % CHUNK == 0 else width
    count = width // size
    loads = [
        pltpu.make_async_copy(source, target, load_sem.at[index])
        for index, (source, target) in enumerate(
            ((down_in, down), (vals_in, vals), (stash_in, stash), (gain_in, gain))
        )
    ]

    def place(index):
        return pl.ds(pl.multiple_of(index * size, size), size)

    def chunks(index):
        at = place(index)
        return [
            pltpu.make_async_copy(source.at[:, :, at], target.at[:, :, at], chunk_sem.at[index, side])
            for side, (source, target) in enumerate(((normed_in, normed), (up_in, up)))
        ]

    for copy in loads[:2]:
        copy.start()
    for index in range(count):
        for copy in chunks(index):
            copy.start()
    for copy in loads[2:]:
        copy.start()
    for copy in loads[:2]:
        copy.wait()

    def step(index, _):
        at = place(index)
        for copy in chunks(index):
            copy.wait()
        for group in range(2):
            value_grad[group, at, :] = (
                transposed_times(normed[group, :, at], down[group]) * grad_scale
            ).astype(jnp.bfloat16)
            pltpu.make_async_copy(
                value_grad.at[group, at, :], value_hbm.at[group, at, :], grad_sem.at[0]
            ).start()
            out_grad[group, :, at] = (
                transposed_times(vals[group], up[group, :, at]) * grad_scale
            ).astype(jnp.bfloat16)
            pltpu.make_async_copy(
                out_grad.at[group, :, at], out_hbm.at[group, :, at], grad_sem.at[1]
            ).start()
        return None

    lax.fori_loop(0, count, step, None)
    small = [
        pltpu.make_async_copy(stash, stash_hbm, small_sem.at[0]),
        pltpu.make_async_copy(gain, gain_hbm, small_sem.at[1]),
    ]
    for load, copy in zip(loads[2:], small):
        load.wait()
        copy.start()
    pltpu.make_async_copy(value_grad, value_hbm, grad_sem.at[0]).wait()
    pltpu.make_async_copy(out_grad, out_hbm, grad_sem.at[1]).wait()
    for copy in small:
        copy.wait()


def final_kernel(own_ref, sent_ref, input_ref, cot_ref, scaled_ref, root_ref, gain_ref, activ_ref, cotan_ref):
    for group in range(2):
        total = own_ref[group].astype(jnp.float32) + sent_ref[group].astype(jnp.float32)
        activ_ref[group] = (input_ref[group].astype(jnp.float32) + total).astype(jnp.bfloat16)
        pulled = own_ref[2 + group].astype(jnp.float32) + sent_ref[2 + group].astype(jnp.float32)
        cotan_ref[group] = input_gradient(
            pulled, cot_ref[group], scaled_ref[group], root_ref[group], gain_ref[pl.ds(group, 1), :]
        )


def relay_body(
    sections,
    w_value,
    w_out,
    norm_gain,
    saved_inputs,
    arriving,
    returning,
    fresh_rows,
    targets,
    fill_slots,
    read_slots,
):
    value_mats, out_mats, gains = w_value[0], w_out[0], norm_gain[0]
    saved, activations, cotangents = saved_inputs[0], arriving[0], returning[0]
    ticks, half, width = fresh_rows.shape
    features = value_mats.shape[2]
    slots = saved.shape[0]
    if slots < 2:
        return body(
            w_value, w_out, norm_gain, saved_inputs, arriving,
            returning, fresh_rows, targets, fill_slots, read_slots,
        )
    rows = 2 * half
    vmem = pl.BlockSpec(memory_space=pltpu.VMEM)
    smem = pl.BlockSpec(memory_space=pltpu.SMEM)
    hbm = pl.BlockSpec(memory_space=pl.ANY)
    shape = jax.ShapeDtypeStruct
    narrow = jnp.bfloat16
    part_shape = shape((4, half, width), narrow)
    (
        part_own, part_peer, inputs, last_cot, scaled, root,
        stash_rows, normed, down, values, upstream, gain_sums,
    ) = pl.pallas_call(
        functools.partial(relay_kernel, sections),
        out_shape=(
            part_shape,
            part_shape,
            shape(activations.shape, narrow),
            shape(cotangents.shape, narrow),
            shape((2, half, width), jnp.float32),
            shape((2, half, 128), jnp.float32),
            shape(saved.shape, narrow),
            shape((2, ticks, 2, half, width), narrow),
            shape((2, ticks, rows, features), narrow),
            shape((2, ticks * rows, features), narrow),
            shape((2, ticks, rows, width), narrow),
            shape(gains.shape, jnp.float32),
        ),
        in_specs=[hbm, hbm, vmem] + [hbm] * 5 + [smem] * 2,
        out_specs=(hbm,) * 12,
        scratch_shapes=[
            pltpu.VMEM(saved.shape, narrow),
            pltpu.VMEM((2, ticks, 2, half, width), narrow),
            pltpu.VMEM((2, ticks, rows, features), narrow),
            pltpu.VMEM((2, ticks * rows, features), narrow),
            pltpu.VMEM((2, ticks, rows, width), narrow),
            pltpu.VMEM((ticks, half, width), narrow),
            pltpu.VMEM(value_mats.shape, narrow),
            pltpu.VMEM(out_mats.shape, narrow),
            pltpu.VMEM((2, features, width), narrow),
            pltpu.VMEM((2, width, features), narrow),
            pltpu.VMEM((ticks, 3, 2, half, width), narrow),
            pltpu.VMEM((ticks, 2, 2, half, width), narrow),
            pltpu.VMEM((slots - 1, 2, half, width), narrow),
            pltpu.VMEM((slots - 1, 2, half, width), narrow),
            pltpu.VMEM((slots, 2, half, width), narrow),
            pltpu.VMEM((ticks, 4, 2, half, width), narrow),
            pltpu.VMEM((ticks, 4, half, width), narrow),
            pltpu.VMEM((ticks, 4, half, width), narrow),
            pltpu.VMEM((rows, width), narrow),
            pltpu.VMEM((2, half, width), jnp.float32),
            pltpu.VMEM((2, half, 128), jnp.float32),
            pltpu.VMEM((2, half, width), jnp.float32),
            pltpu.VMEM((2, 1, width), jnp.float32),
            pltpu.VMEM((2, 1, width), jnp.float32),
            pltpu.SemaphoreType.DMA((2, 2)),
            pltpu.SemaphoreType.DMA((7,)),
            pltpu.SemaphoreType.DMA((15,)),
            pltpu.SemaphoreType.DMA((ticks, 4)),
            pltpu.SemaphoreType.DMA((ticks, 4)),
            pltpu.SemaphoreType.DMA((ticks, 4, 2)),
            pltpu.SemaphoreType.DMA((ticks, 4, 2)),
            pltpu.SemaphoreType.DMA((slots - 1, 2)),
            pltpu.SemaphoreType.DMA((slots - 1, 2)),
            pltpu.SemaphoreType.DMA((ticks,)),
            pltpu.SemaphoreType.DMA((ticks,)),
            pltpu.SemaphoreType.DMA((2, 2)),
        ],
        compiler_params=pltpu.CompilerParams(
            collective_id=0, has_side_effects=True, vmem_limit_bytes=VMEM_GRANT
        ),
    )(
        value_mats, out_mats, gains, saved, activations, cotangents,
        fresh_rows, targets, fill_slots[0].T, read_slots[0].T,
    )
    part_sent = shifted(part_peer, "dp", 1)
    flat = lambda block: block.reshape(2, ticks * rows, block.shape[-1])
    operands = (stash_rows, gain_sums, flat(normed), flat(down), values, flat(upstream))
    stash_out, value_grad, out_grad, gain_grad = pl.pallas_call(
        functools.partial(grads_kernel, (ticks * rows) ** (-0.5)),
        out_shape=(
            shape(saved.shape, narrow),
            shape(value_mats.shape, narrow),
            shape(out_mats.shape, narrow),
            shape(gains.shape, jnp.float32),
        ),
        in_specs=[hbm] * 6,
        out_specs=(hbm,) * 4,
        scratch_shapes=[pltpu.VMEM(block.shape, block.dtype) for block in operands] + [
            pltpu.VMEM(value_mats.shape, narrow),
            pltpu.VMEM(out_mats.shape, narrow),
            pltpu.SemaphoreType.DMA((4,)),
            pltpu.SemaphoreType.DMA((width // CHUNK if width % CHUNK == 0 else 1, 2)),
            pltpu.SemaphoreType.DMA((2,)),
            pltpu.SemaphoreType.DMA((2,)),
        ],
        compiler_params=pltpu.CompilerParams(vmem_limit_bytes=WHOLE_VMEM),
        cost_estimate=pl.CostEstimate(
            flops=32 * ticks * rows * width * features, bytes_accessed=8 * width * features, transcendentals=0
        ),
    )(*operands)
    final_rows, gradients = pl.pallas_call(
        final_kernel,
        out_shape=(shape(activations.shape, narrow), shape(cotangents.shape, narrow)),
        in_specs=[vmem] * 7,
        out_specs=(vmem,) * 2,
    )(part_own, part_sent, inputs, last_cot, scaled, root, gains)
    results = (final_rows, gradients, stash_out, value_grad, out_grad, gain_grad)
    return tuple(block[None] for block in results)


def solution(mesh):
    in_specs = (
        P("section", None, None, "dp"),
        P("section", None, "dp", None),
        P("section", None, None),
        P("section", None, None, "dp", None),
        P("section", None, "dp", None),
        P("section", None, "dp", None),
        P(None, "dp", None),
        P(None, "dp", None),
        P("section", None, None),
        P("section", None, None),
    )
    out_specs = (
        P("section", None, "dp", None),
        P("section", None, "dp", None),
        P("section", None, None, "dp", None),
        P("section", None, None, "dp"),
        P("section", None, "dp", None),
        P("section", None, None),
    )
    paired = mesh.shape["dp"] == 2 and mesh.shape["section"] > 2
    program = functools.partial(relay_body, mesh.shape["section"]) if paired else body
    return jax.shard_map(program, mesh=mesh, in_specs=in_specs, out_specs=out_specs, check_vma=False)
```
